32 devices in a mesh: slab: 8 (over y, x, core), tm: 4 (over z).
Axes of the slice: x: 2, y: 2, z: 4, core: 2. Of those that a mesh axis runs over, the one named last changes fastest.
Arguments:
- field: float32 [2, 128, 256, 512], P(None, 'slab', None, 'tm'), may hold values from -110 to 110
Outputs:
- evolved: float32 [2, 128, 256, 512], P(None, 'slab', None, 'tm')
The draws below stay inside these ranges and needn't reach their ends.
All inputs are finite; a program needn't handle non-finite values.
Results may differ from the reference program's by a relative error of at most 0.000098.
Values sent between devices are 32-bit elements; how exact they have to be, the bound alone decides.
A program may use at most 128 MiB of HBM per device.

```python
import math
import jax
import jax.numpy as jnp
from jax import lax

NX = 128
NY = 256
NT = 512


def draw_field(key, part):
    key_rows = jax.random.fold_in(key, 11)
    key_times = jax.random.fold_in(key, 23)
    key_entries = jax.random.fold_in(key, 37)
    log_ten = math.log(10.0)
    rising = 1.0 + 2.0 * jnp.arange(NX, dtype=jnp.float32) / NX
    row_scale = jnp.exp(jax.random.uniform(key_rows, (NX,), jnp.float32, 0.0, log_ten)) * rising
    time_scale = jnp.exp(jax.random.uniform(key_times, (NT,), jnp.float32, 0.0, log_ten))
    entries = jnp.clip(jax.random.normal(key_entries, (2, NX, NY, NT), jnp.float32), -6.0, 6.0)
    amplitude = jnp.sqrt(row_scale[:, None, None] * time_scale[None, None, :])
    return entries * amplitude[None]


def setup_inputs(seed: int = 0) -> dict:
    arg_keys = jax.random.split(jax.random.key(seed), 2)
    field = draw_field(jax.random.fold_in(arg_keys[1], 71), 0)
    return dict(field=field)


TWO_PI = 2.0 * math.pi
DIFFRACT = 4.0
DISPERSE = 3.0
KERR = 0.05
WELL = 1.5
EPSILON = 1e-06

def frequency(length):
    positions = jnp.arange(length, dtype=jnp.int32)
    signed = jnp.where(2 * positions < length, positions, positions - length)
    return signed.astype(jnp.float32) * (TWO_PI / length)

def reference(field):
    mean_power = jnp.mean(field[0] * field[0] + field[1] * field[1])
    launch_scale = 1.0 / jnp.sqrt(mean_power + EPSILON)
    launched = lax.complex(field[0] * launch_scale, field[1] * launch_scale)
    across_x = frequency(NX)
    across_y = frequency(NY)
    temporal = frequency(NT)
    theta = -DIFFRACT * (across_x[:, None, None] ** 2 + across_y[None, :, None] ** 2) + DISPERSE * temporal[None, None, :] ** 2
    rotor = lax.complex(jnp.cos(theta), jnp.sin(theta))

    def half_step(wave):
        return jnp.fft.ifftn(jnp.fft.fftn(wave, axes=(0, 1, 2)) * rotor, axes=(0, 1, 2))
    after_half = half_step(launched)
    place_x = (jnp.arange(NX, dtype=jnp.float32) - (NX - 1) / 2.0) / (NX / 2.0)
    place_y = (jnp.arange(NY, dtype=jnp.float32) - (NY - 1) / 2.0) / (NY / 2.0)
    well_depth = WELL * (place_x[:, None, None] ** 2 + place_y[None, :, None] ** 2)
    intensity = jnp.real(after_half) ** 2 + jnp.imag(after_half) ** 2
    kick_angle = KERR * intensity - well_depth
    kicked = after_half * lax.complex(jnp.cos(kick_angle), jnp.sin(kick_angle))
    evolved = half_step(kicked)
    return jnp.stack([jnp.real(evolved), jnp.imag(evolved)])
```

```python
import math

import numpy as np

import jax
import jax.numpy as jnp
from jax import lax
from jax.sharding import PartitionSpec as P

TWO_PI = 2.0 * math.pi
DIFFRACT = 4.0
DISPERSE = 3.0
KERR = 0.05
WELL = 1.5
EPSILON = 1e-06
AXES = ("slab", "tm")
CHUNKS = 2


def propagator(length, strength):
    steps = np.arange(length)
    signed = np.where(2 * steps < length, steps, steps - length)
    phase = np.exp(1j * strength * (TWO_PI * signed / length) ** 2)
    response = np.fft.ifft(phase)
    matrix = response[(steps[:, None] - steps[None, :]) % length]
    real = jnp.asarray(matrix.real.astype(np.float32))
    imag = jnp.asarray(matrix.imag.astype(np.float32))
    upper = jnp.stack([real, -imag], axis=1)
    lower = jnp.stack([imag, real], axis=1)
    return jnp.stack([upper, lower])


def apply(form, table, value):
    return jnp.einsum(form, table, value, precision=lax.Precision.HIGH)


def place(index, length):
    return (index.astype(jnp.float32) - (length - 1) / 2.0) / (length / 2.0)


def kick(real, imag, scale, well_depth):
    real = real * scale
    imag = imag * scale
    angle = KERR * (real * real + imag * imag) - well_depth
    turn_c = jnp.cos(angle)
    turn_s = jnp.sin(angle)
    return real * turn_c - imag * turn_s, real * turn_s + imag * turn_c


def on_device(field):
    slabs = lax.axis_size("slab")
    times = lax.axis_size("tm")
    devices = slabs * times
    _, rows, ny, cols = field.shape
    nx = rows * slabs
    nt = cols * times
    along_x = propagator(nx, -DIFFRACT)
    along_y = propagator(ny, -DIFFRACT)
    along_t = propagator(nt, DISPERSE)
    partial_power = jnp.sum(field[0] * field[0] + field[1] * field[1])
    mean_power = lax.psum(partial_power, AXES) / (nx * ny * nt)
    scale = 1.0 / jnp.sqrt(mean_power + EPSILON)
    index_x = jnp.arange(nx, dtype=jnp.int32)

    if ny % devices == 0:
        group = ny // devices
        chunks = math.gcd(group, CHUNKS)
        piece = group // chunks
        spread = along_y.reshape(2, devices, chunks, piece, 2, ny)
        gather = along_y.reshape(2, ny, 2, devices, chunks, piece)
        arrived = []
        for chunk in range(chunks):
            table = spread[:, :, chunk].reshape(2, devices * piece, 2, ny)
            sent = apply("qzpb,pabc->zqac", table, field)
            if chunk == 0:
                sent, scale = lax.optimization_barrier((sent, scale))
            arrived.append(
                lax.all_to_all(sent, AXES, split_axis=0, concat_axis=0, tiled=True)
            )
        total = None
        for chunk in range(chunks):
            got = arrived[chunk].reshape(slabs, times, piece, 2, rows, cols)
            mixed = apply("qxpsa,smgpac->gqxmc", along_x.reshape(2, nx, 2, slabs, rows), got)
            whole = apply("rtqT,gqxT->grxt", along_t, mixed.reshape(piece, 2, nx, nt))
            first = lax.axis_index(AXES) * group + chunk * piece
            place_y = place(first + jnp.arange(piece, dtype=jnp.int32), ny)
            well_depth = WELL * (
                place(index_x, nx)[None, :, None] ** 2 + place_y[:, None, None] ** 2
            )
            kicked = jnp.stack(kick(whole[:, 0], whole[:, 1], scale, well_depth), axis=1)
            timed = apply("rtqT,gqxT->grxt", along_t, kicked)
            back = apply(
                "qsapX,gpXmc->smgqac",
                along_x.reshape(2, slabs, rows, 2, nx),
                timed.reshape(piece, 2, nx, times, cols),
            )
            home = lax.all_to_all(
                back.reshape(devices * piece, 2, rows, cols),
                AXES,
                split_axis=0,
                concat_axis=0,
                tiled=True,
            )
            table = gather[:, :, :, :, chunk].reshape(2, ny, 2, devices * piece)
            part = apply("qzpb,bpac->qazc", table, home)
            total = part if total is None else total + part
        return total

    group = ny // times
    width = group * nt // slabs
    sent = apply("qzpb,pabc->qazc", along_y, field)
    timed = lax.all_to_all(sent, "tm", split_axis=2, concat_axis=3, tiled=True)
    timed = apply("rtqT,qabT->rabt", along_t, timed)
    crossed = lax.all_to_all(
        timed.reshape(2, rows, slabs, width), "slab", split_axis=2, concat_axis=1, tiled=True
    ).reshape(2, nx, width)
    crossed = apply("qxpX,pXw->qxw", along_x, crossed)
    flat = lax.axis_index("slab") * width + jnp.arange(width, dtype=jnp.int32)
    place_y = place(lax.axis_index("tm") * group + flat // nt, ny)
    well_depth = WELL * (place(index_x, nx)[:, None] ** 2 + place_y[None, :] ** 2)
    kicked = jnp.stack(kick(crossed[0], crossed[1], scale, well_depth))
    kicked = apply("qxpX,pXw->qxw", along_x, kicked)
    timed = lax.all_to_all(
        kicked.reshape(2, nx, 1, width), "slab", split_axis=1, concat_axis=2, tiled=True
    ).reshape(2, rows, group, nt)
    timed = apply("rtqT,qabT->rabt", along_t, timed)
    home = lax.all_to_all(timed, "tm", split_axis=3, concat_axis=2, tiled=True)
    return apply("qzpb,pabc->qazc", along_y, home)


def solution(mesh):
    placed = (P(None, "slab", None, "tm"),)
    return jax.shard_map(
        on_device,
        mesh=mesh,
        in_specs=placed,
        out_specs=P(None, "slab", None, "tm"),
        check_vma=False,
    )
```

```python
import functools
import math

import ml_dtypes
import numpy as np

import jax
import jax.numpy as jnp
from jax import lax
from jax.experimental import pallas as pl
from jax.experimental.pallas import tpu as pltpu
from jax.sharding import PartitionSpec as P

TWO_PI = 2.0 * math.pi
DIFFRACT = 4.0
DISPERSE = 3.0
KERR = 0.05
WELL = 1.5
EPSILON = 1e-06
AXES = ("slab", "tm")
PIECE = 1
LANES = 128
WIDE = 256
MESH = pl.DeviceIdType.MESH


def matrix(length, strength):
    steps = np.arange(length)
    signed = np.where(2 * steps < length, steps, steps - length)
    phase = np.exp(1j * strength * (TWO_PI * signed / length) ** 2)
    response = np.fft.ifft(phase)
    return response[(steps[:, None] - steps[None, :]) % length]


def propagator(length, strength):
    whole = matrix(length, strength)
    real = jnp.asarray(whole.real.astype(np.float32))
    imag = jnp.asarray(whole.imag.astype(np.float32))
    upper = jnp.stack([real, -imag], axis=1)
    lower = jnp.stack([imag, real], axis=1)
    return jnp.stack([upper, lower])


def halves(table):
    table = table.astype(np.float32)
    high = table.astype(ml_dtypes.bfloat16)
    low = (table - high.astype(np.float32)).astype(ml_dtypes.bfloat16)
    return high, low


def blocks(whole):
    return np.block([[whole.real, -whole.imag], [whole.imag, whole.real]])


def apply(form, table, value):
    return jnp.einsum(form, table, value, precision=lax.Precision.HIGH)


def place(index, length):
    return (index.astype(jnp.float32) - (length - 1) / 2.0) / (length / 2.0)


def kick(real, imag, scale, well_depth):
    real = real * scale
    imag = imag * scale
    angle = KERR * (real * real + imag * imag) - well_depth
    turn_c = jnp.cos(angle)
    turn_s = jnp.sin(angle)
    return real * turn_c - imag * turn_s, real * turn_s + imag * turn_c


def split(value):
    high = value.astype(jnp.bfloat16)
    low = (value - high.astype(jnp.float32)).astype(jnp.bfloat16)
    return high, low


def dot(left, right):
    return jnp.dot(left, right, preferred_element_type=jnp.float32)


def left_table(table, high, low):
    n = table.shape[0] // 2
    both = dot(table, high)
    return both[:n] + both[n:] + dot(table[:n], low)


def step_kernel(
    dims,
    field_ref,
    fwd_ref,
    across_ref,
    time_ref,
    back_ref,
    out_ref,
    fld,
    fh,
    fl,
    fwd,
    across,
    wt,
    back,
    turn,
    send,
    recv,
    xh,
    xl,
    ysp,
    ksp,
    hsend,
    home,
    acc,
    pw_send,
    pw_recv,
    load_sem,
    table_sem,
    out_sem,
    send_sem,
    recv_sem,
    hsend_sem,
    home_sem,
    pw_sem,
):
    slabs, times, rows, ny, cols, piece, chunks = dims
    devices = slabs * times
    nx, nt = slabs * rows, times * cols
    group = devices * piece
    blk = piece * 2 * rows
    pitch = turn.shape[0] // rows
    pairs = rows // 2
    s = lax.axis_index("slab")
    m = lax.axis_index("tm")
    me = s * times + m

    def field_copy(xp):
        part = (slice(None), pl.ds(2 * xp, 2))
        return pltpu.make_async_copy(field_ref.at[part], fld.at[part], load_sem.at[xp])

    for xp in range(pairs):
        field_copy(xp).start()
    tables = [
        pltpu.make_async_copy(a, b, table_sem.at[i])
        for i, (a, b) in enumerate(
            [(fwd_ref, fwd), (across_ref, across), (time_ref, wt), (back_ref, back)]
        )
    ]
    for copy in tables:
        copy.start()

    barrier = pltpu.get_barrier_semaphore()

    def greet(k, carry):
        peer = (me + k) % devices
        pl.semaphore_signal(
            barrier, inc=1, device_id=(peer // times, peer % times), device_id_type=MESH
        )
        return carry

    lax.fori_loop(1, devices, greet, 0)

    def prepare(xp, total):
        field_copy(xp).wait()
        for q in range(2):
            value = jnp.concatenate([fld[q, 2 * xp], fld[q, 2 * xp + 1]], axis=1)
            high, low = split(value)
            fh[xp, pl.ds(q * ny, ny), :] = high
            fl[xp, pl.ds(q * ny, ny), :] = low
            total = total + jnp.sum((value * value).reshape(ny // 8, 8, 2 * cols), axis=0)
        return total

    total = lax.fori_loop(0, pairs, prepare, jnp.zeros((8, 2 * cols), jnp.float32))
    total = total[:, :cols] + total[:, cols:]
    pw_send[...] = total
    pw_recv[me] = total

    half = times // 2
    side = m // half
    order = []
    for i in range(half):
        order.append([(1 - side) * half + (m + i) % half, False])
    for i in range(1, half):
        order.append([side * half + (m + i) % half, False])
    order.append([m, True])

    def to_all(make):
        for there, own in order:
            for k in range(slabs):
                if own and k == 0:
                    continue
                make((s + k) % slabs, there)

    def forward_copy(c, ds, dm):
        return pltpu.make_async_remote_copy(
            src_ref=send.at[c, pl.ds((ds * times + dm) * blk, blk)],
            dst_ref=recv.at[c, pl.ds(me * blk, blk)],
            send_sem=send_sem.at[c],
            recv_sem=recv_sem.at[c],
            device_id=(ds, dm),
            device_id_type=MESH,
        )

    def home_copy(c, ds, dm):
        return pltpu.make_async_remote_copy(
            src_ref=hsend.at[c, pl.ds((ds * times + dm) * blk, blk)],
            dst_ref=home.at[c, pl.ds(me * blk, blk)],
            send_sem=hsend_sem.at[c],
            recv_sem=home_sem.at[c],
            device_id=(ds, dm),
            device_id_type=MESH,
        )

    def power_copy(ds, dm):
        return pltpu.make_async_remote_copy(
            src_ref=pw_send,
            dst_ref=pw_recv.at[me],
            send_sem=pw_sem.at[0],
            recv_sem=pw_sem.at[1],
            device_id=(ds, dm),
            device_id_type=MESH,
        )

    def whole(src, dst, first, second):
        return pltpu.make_async_remote_copy(
            src_ref=src,
            dst_ref=dst,
            send_sem=first,
            recv_sem=second,
            device_id=(s, m),
            device_id_type=MESH,
        )

    others = pl.ds(0, (devices - 1) * blk)

    def spread(c):
        def along_y(xp, carry):
            result = left_table(fwd[c], fh[xp], fl[xp])
            turn[pl.ds(2 * xp * pitch, 2 * group), :] = result[:, :cols]
            turn[pl.ds((2 * xp + 1) * pitch, 2 * group), :] = result[:, cols:]
            return carry

        lax.fori_loop(0, pairs, along_y, 0)
        for r in range(group):
            for q in range(2):
                send[c, pl.ds((r * 2 + q) * rows, rows), :] = turn[
                    pl.ds(q * group + r, rows, stride=pitch), :
                ]
        for j in range(piece):
            for q in range(2):
                recv[c, pl.ds(me * blk + (j * 2 + q) * rows, rows), :] = turn[
                    pl.ds(q * group + me * piece + j, rows, stride=pitch), :
                ]

    tables[0].wait()
    spread(0)
    pl.semaphore_wait(barrier, devices - 1)
    to_all(lambda ds, dm: forward_copy(0, ds, dm).start())
    to_all(lambda ds, dm: power_copy(ds, dm).start())

    def rest(c, carry):
        spread(c)
        to_all(lambda ds, dm: forward_copy(c, ds, dm).start())
        return carry

    lax.fori_loop(1, chunks, rest, 0)

    for copy in tables[1:]:
        copy.wait()
    whole(pw_recv.at[pl.ds(0, devices - 1)], pw_recv.at[pl.ds(0, devices - 1)], pw_sem.at[0], pw_sem.at[1]).wait_recv()
    power = jnp.sum(jnp.sum(pw_recv[...], axis=0), axis=(0, 1), keepdims=True)
    scale = 1.0 / jnp.sqrt(power / (nx * ny * nt) + EPSILON)
    place_x = place(lax.broadcasted_iota(jnp.int32, (nx, WIDE), 0), nx)
    square_x = place_x * place_x
    tiles = nt // WIDE
    per_tile = WIDE // cols

    def along_t(source, n):
        lanes = pl.ds(n * WIDE, WIDE)
        parts = []
        for part in range(2):
            both = dot(source[...], wt[part, 0, :, lanes])
            parts.append(
                both[: 2 * nx] + both[2 * nx :] + dot(source[: 2 * nx], wt[part, 1, :, lanes])
            )
        gr, gi = parts
        return gr[:nx] - gi[nx:], gi[:nx] + gr[nx:]

    def middle(c, carry):
        whole(recv.at[c, others], recv.at[c, others], send_sem.at[c], recv_sem.at[c]).wait_recv()
        for j in range(piece):
            for a in range(slabs):
                for b in range(times):
                    for q in range(2):
                        got = recv[
                            c, pl.ds((a * times + b) * blk + (j * 2 + q) * rows, rows), :
                        ]
                        high, low = split(got)
                        xh[pl.ds(q * nx + a * rows, rows), pl.ds(b * cols, cols)] = high
                        xl[pl.ds(q * nx + a * rows, rows), pl.ds(b * cols, cols)] = low
            for n in range(tiles):
                lanes = pl.ds(n * WIDE, WIDE)
                value = left_table(across[...], xh[:, lanes], xl[:, lanes])
                high, low = split(value)
                ysp[pl.ds(0, 2 * nx), lanes] = high
                ysp[pl.ds(2 * nx, 2 * nx), lanes] = low
            y = c * group + me * piece + j
            place_y = (y.astype(jnp.float32) - (ny - 1) / 2.0) / (ny / 2.0)
            well_depth = WELL * (square_x + place_y * place_y)
            for n in range(tiles):
                lanes = pl.ds(n * WIDE, WIDE)
                real, imag = along_t(ysp, n)
                real, imag = kick(real, imag, scale, well_depth)
                for q, value in enumerate((real, imag)):
                    high, low = split(value)
                    ksp[pl.ds(q * nx, nx), lanes] = high
                    ksp[pl.ds((2 + q) * nx, nx), lanes] = low
            for n in range(tiles):
                lanes = pl.ds(n * WIDE, WIDE)
                for q, value in enumerate(along_t(ksp, n)):
                    high, low = split(value)
                    xh[pl.ds(q * nx, nx), lanes] = high
                    xl[pl.ds(q * nx, nx), lanes] = low
            for n in range(tiles):
                lanes = pl.ds(n * WIDE, WIDE)
                value = left_table(across[...], xh[:, lanes], xl[:, lanes])
                for q in range(2):
                    for a in range(slabs):
                        for b in range(per_tile):
                            dest = a * times + n * per_tile + b
                            hsend[c, pl.ds(dest * blk + (j * 2 + q) * rows, rows), :] = value[
                                q * nx + a * rows : q * nx + (a + 1) * rows,
                                b * cols : (b + 1) * cols,
                            ]
        home[c, pl.ds(me * blk, blk), :] = hsend[c, pl.ds(me * blk, blk), :]
        to_all(lambda ds, dm: home_copy(c, ds, dm).start())
        return carry

    lax.fori_loop(0, chunks, middle, 0)

    def gather(c, last):
        whole(home.at[c, others], home.at[c, others], hsend_sem.at[c], home_sem.at[c]).wait_recv()

        def along_y(xp, carry):
            sides = []
            for i in range(2):
                sides.append(
                    jnp.concatenate(
                        [
                            home[c, pl.ds(q * rows + 2 * xp + i, group, stride=2 * rows), :]
                            for q in range(2)
                        ],
                        axis=0,
                    )
                )
            high, low = split(jnp.concatenate(sides, axis=1))
            value = left_table(back[c], high, low)
            for q in range(2):
                for i in range(2):
                    part = value[q * ny : (q + 1) * ny, i * cols : (i + 1) * cols]
                    acc[q, 2 * xp + i] = acc[q, 2 * xp + i] + part
            if last:
                out_copy(xp).start()
            return carry

        lax.fori_loop(0, pairs, along_y, 0)

    def out_copy(xp):
        part = (slice(None), pl.ds(2 * xp, 2))
        return pltpu.make_async_copy(acc.at[part], out_ref.at[part], out_sem.at[xp])

    acc[...] = jnp.zeros_like(acc)

    def early(c, carry):
        gather(c, False)
        return carry

    lax.fori_loop(0, chunks - 1, early, 0)
    gather(chunks - 1, True)

    def drain(c, carry):
        whole(send.at[c, others], send.at[c, others], send_sem.at[c], recv_sem.at[c]).wait_send()
        whole(hsend.at[c, others], hsend.at[c, others], hsend_sem.at[c], home_sem.at[c]).wait_send()
        return carry

    lax.fori_loop(0, chunks, drain, 0)
    whole(pw_recv.at[pl.ds(0, devices - 1)], pw_recv.at[pl.ds(0, devices - 1)], pw_sem.at[0], pw_sem.at[1]).wait_send()
    for xp in range(pairs):
        out_copy(xp).wait()


def in_one_kernel(field, slabs, times, piece):
    _, rows, ny, cols = field.shape
    devices = slabs * times
    nx, nt = rows * slabs, cols * times
    group = devices * piece
    chunks = ny // group
    blk = piece * 2 * rows
    pitch = 2 * group + 8
    uy = matrix(ny, -DIFFRACT)
    ux = matrix(nx, -DIFFRACT)
    ut = matrix(nt, DISPERSE)
    full_y = blocks(uy).reshape(2, ny, 2, ny)
    fwd = np.stack(
        [
            np.concatenate(halves(full_y[:, c * group : (c + 1) * group].reshape(2 * group, 2 * ny)))
            for c in range(chunks)
        ]
    )
    back = np.stack(
        [
            np.concatenate(
                halves(full_y[:, :, :, c * group : (c + 1) * group].reshape(2 * ny, 2 * group))
            )
            for c in range(chunks)
        ]
    )
    across = np.concatenate(halves(blocks(ux)))
    time = np.stack([np.stack(halves(ut.real)), np.stack(halves(ut.imag))])
    dims = (slabs, times, rows, ny, cols, piece, chunks)
    f32, bf16 = jnp.float32, jnp.bfloat16
    any_space = pl.BlockSpec(memory_space=pl.ANY)
    dma = pltpu.SemaphoreType.DMA
    return pl.pallas_call(
        functools.partial(step_kernel, dims),
        out_shape=jax.ShapeDtypeStruct(field.shape, f32),
        in_specs=[any_space] * 5,
        out_specs=any_space,
        scratch_shapes=[
            pltpu.VMEM(field.shape, f32),
            pltpu.VMEM((rows // 2, 2 * ny, 2 * cols), bf16),
            pltpu.VMEM((rows // 2, 2 * ny, 2 * cols), bf16),
            pltpu.VMEM(fwd.shape, bf16),
            pltpu.VMEM(across.shape, bf16),
            pltpu.VMEM(time.shape, bf16),
            pltpu.VMEM(back.shape, bf16),
            pltpu.VMEM((rows * pitch, cols), f32),
            pltpu.VMEM((chunks, devices * blk, cols), f32),
            pltpu.VMEM((chunks, devices * blk, cols), f32),
            pltpu.VMEM((2 * nx, nt), bf16),
            pltpu.VMEM((2 * nx, nt), bf16),
            pltpu.VMEM((4 * nx, nt), bf16),
            pltpu.VMEM((4 * nx, nt), bf16),
            pltpu.VMEM((chunks, devices * blk, cols), f32),
            pltpu.VMEM((chunks, devices * blk, cols), f32),
            pltpu.VMEM(field.shape, f32),
            pltpu.VMEM((8, cols), f32),
            pltpu.VMEM((devices, 8, cols), f32),
            dma((rows // 2,)),
            dma((4,)),
            dma((rows // 2,)),
            dma((chunks,)),
            dma((chunks,)),
            dma((chunks,)),
            dma((chunks,)),
            dma((2,)),
        ],
        compiler_params=pltpu.CompilerParams(
            collective_id=0, has_side_effects=True, vmem_limit_bytes=60 * 1024 * 1024
        ),
    )(field, jnp.asarray(fwd), jnp.asarray(across), jnp.asarray(time), jnp.asarray(back))


def on_device(field):
    slabs = lax.axis_size("slab")
    times = lax.axis_size("tm")
    devices = slabs * times
    _, rows, ny, cols = field.shape
    nx = rows * slabs
    nt = cols * times
    if (
        ny % (devices * PIECE) == 0
        and rows % 16 == 0
        and cols == LANES
        and nt % WIDE == 0
        and times % 2 == 0
    ):
        return in_one_kernel(field, slabs, times, PIECE)

    along_x = propagator(nx, -DIFFRACT)
    along_y = propagator(ny, -DIFFRACT)
    along_t = propagator(nt, DISPERSE)
    partial_power = jnp.sum(field[0] * field[0] + field[1] * field[1])
    mean_power = lax.psum(partial_power, AXES) / (nx * ny * nt)
    scale = 1.0 / jnp.sqrt(mean_power + EPSILON)
    index_x = jnp.arange(nx, dtype=jnp.int32)
    group = ny // times
    width = group * nt // slabs
    sent = apply("qzpb,pabc->qazc", along_y, field)
    timed = lax.all_to_all(sent, "tm", split_axis=2, concat_axis=3, tiled=True)
    timed = apply("rtqT,qabT->rabt", along_t, timed)
    crossed = lax.all_to_all(
        timed.reshape(2, rows, slabs, width), "slab", split_axis=2, concat_axis=1, tiled=True
    ).reshape(2, nx, width)
    crossed = apply("qxpX,pXw->qxw", along_x, crossed)
    flat = lax.axis_index("slab") * width + jnp.arange(width, dtype=jnp.int32)
    place_y = place(lax.axis_index("tm") * group + flat // nt, ny)
    well_depth = WELL * (place(index_x, nx)[:, None] ** 2 + place_y[None, :] ** 2)
    kicked = jnp.stack(kick(crossed[0], crossed[1], scale, well_depth))
    kicked = apply("qxpX,pXw->qxw", along_x, kicked)
    timed = lax.all_to_all(
        kicked.reshape(2, nx, 1, width), "slab", split_axis=1, concat_axis=2, tiled=True
    ).reshape(2, rows, group, nt)
    timed = apply("rtqT,qabT->rabt", along_t, timed)
    home = lax.all_to_all(timed, "tm", split_axis=3, concat_axis=2, tiled=True)
    return apply("qzpb,pabc->qazc", along_y, home)


def solution(mesh):
    placed = (P(None, "slab", None, "tm"),)
    return jax.shard_map(
        on_device,
        mesh=mesh,
        in_specs=placed,
        out_specs=P(None, "slab", None, "tm"),
        check_vma=False,
    )
```

```python
import functools
import math

import ml_dtypes
import numpy as np

import jax
import jax.numpy as jnp
from jax import lax
from jax.experimental import pallas as pl
from jax.experimental.pallas import tpu as pltpu
from jax.sharding import PartitionSpec as P

TWO_PI = 2.0 * math.pi
DIFFRACT = 4.0
DISPERSE = 3.0
KERR = 0.05
WELL = 1.5
EPSILON = 1e-06
AXES = ("slab", "tm")
LANES = 128
WIDE = 256
MESH = pl.DeviceIdType.MESH


def matrix(length, strength):
    steps = np.arange(length)
    signed = np.where(2 * steps < length, steps, steps - length)
    phase = np.exp(1j * strength * (TWO_PI * signed / length) ** 2)
    response = np.fft.ifft(phase)
    return response[(steps[:, None] - steps[None, :]) % length]


def propagator(length, strength):
    whole = matrix(length, strength)
    real = jnp.asarray(whole.real.astype(np.float32))
    imag = jnp.asarray(whole.imag.astype(np.float32))
    upper = jnp.stack([real, -imag], axis=1)
    lower = jnp.stack([imag, real], axis=1)
    return jnp.stack([upper, lower])


def halves(table):
    table = table.astype(np.float32)
    high = table.astype(ml_dtypes.bfloat16)
    low = (table - high.astype(np.float32)).astype(ml_dtypes.bfloat16)
    return high, low


def blocks(whole):
    return np.block([[whole.real, -whole.imag], [whole.imag, whole.real]])


def apply(form, table, value):
    return jnp.einsum(form, table, value, precision=lax.Precision.HIGH)


def place(index, length):
    return (index.astype(jnp.float32) - (length - 1) / 2.0) / (length / 2.0)


def kick(real, imag, scale, well_depth):
    real = real * scale
    imag = imag * scale
    angle = KERR * (real * real + imag * imag) - well_depth
    turn_c = jnp.cos(angle)
    turn_s = jnp.sin(angle)
    return real * turn_c - imag * turn_s, real * turn_s + imag * turn_c


def split(value):
    high = value.astype(jnp.bfloat16)
    low = (value - high.astype(jnp.float32)).astype(jnp.bfloat16)
    return high, low


def dot(left, right):
    return jnp.dot(left, right, preferred_element_type=jnp.float32)


def left_table(table, high, low):
    n = table.shape[0] // 2
    both = dot(table, high)
    return both[:n] + both[n:] + dot(table[:n], low)


def stacked_table(table, high, low):
    return dot(table, jnp.concatenate([high, high, low], axis=0))


def home_pair(home, start, pitch, group, rows):
    sides = []
    for i in range(2):
        sides.append(
            jnp.concatenate(
                [home[pl.ds(start + q * 8 + i, group, stride=pitch), :] for q in range(2)],
                axis=0,
            )
        )
    return split(jnp.concatenate(sides, axis=1))


def step_kernel(
    dims,
    field_ref,
    fwd_ref,
    across_ref,
    time_ref,
    back_ref,
    acc,
    home_last,
    fld,
    fh,
    fl,
    fwd,
    across,
    wt,
    back,
    turn,
    send,
    recv,
    xh,
    xl,
    ysp,
    ksp,
    hsend,
    home,
    pw_send,
    pw_recv,
    load_sem,
    table_sem,
    send_sem,
    recv_sem,
    hsend_sem,
    home_sem,
    last_sem,
    pw_sem,
):
    slabs, times, rows, ny, cols, chunks = dims
    group = slabs * times
    nx, nt = slabs * rows, times * cols
    blk = 2 * rows
    pitch = turn.shape[0] // rows
    hpitch = home_last.shape[0] // group
    pairs = rows // 2
    s = lax.axis_index("slab")
    m = lax.axis_index("tm")
    me = s * times + m

    def field_copy(xp):
        part = (slice(None), pl.ds(2 * xp, 2))
        return pltpu.make_async_copy(field_ref.at[part], fld.at[part], load_sem.at[xp])

    rest_rows = pl.ds(1, chunks - 1)
    tables = [
        pltpu.make_async_copy(a, b, table_sem.at[i])
        for i, (a, b) in enumerate(
            [
                (fwd_ref.at[0], fwd.at[0]),
                (fwd_ref.at[rest_rows], fwd.at[rest_rows]),
                (across_ref, across),
                (time_ref, wt),
                (back_ref, back),
            ]
        )
    ]
    tables[0].start()
    for xp in range(pairs):
        field_copy(xp).start()

    barrier = pltpu.get_barrier_semaphore()

    def greet(k, carry):
        peer = (me + k) % group
        pl.semaphore_signal(
            barrier, inc=1, device_id=(peer // times, peer % times), device_id_type=MESH
        )
        return carry

    lax.fori_loop(1, group, greet, 0)

    half = times // 2
    side = m // half
    order = []
    for i in range(half):
        order.append([(1 - side) * half + (m + i) % half, False])
    for i in range(1, half):
        order.append([side * half + (m + i) % half, False])
    order.append([m, True])

    def to_all(make):
        for there, own in order:
            for k in range(slabs):
                if own and k == 0:
                    continue
                make((s + k) % slabs, there)

    def forward_copy(c, ds, dm, first, count):
        return pltpu.make_async_remote_copy(
            src_ref=send.at[c, pl.ds((ds * times + dm) * blk + first, count)],
            dst_ref=recv.at[c, pl.ds(me * blk + first, count)],
            send_sem=send_sem.at[c],
            recv_sem=recv_sem.at[c],
            device_id=(ds, dm),
            device_id_type=MESH,
        )

    def home_copy(c, ds, dm):
        return pltpu.make_async_remote_copy(
            src_ref=hsend.at[c, pl.ds((ds * times + dm) * blk, blk)],
            dst_ref=home.at[c, pl.ds(me * hpitch, blk)],
            send_sem=hsend_sem.at[c],
            recv_sem=home_sem.at[c],
            device_id=(ds, dm),
            device_id_type=MESH,
        )

    def last_copy(h, ds, dm):
        return pltpu.make_async_remote_copy(
            src_ref=hsend.at[chunks - 1, pl.ds((ds * times + dm) * blk + h * rows, rows)],
            dst_ref=home_last.at[pl.ds(me * hpitch + h * rows, rows)],
            send_sem=hsend_sem.at[chunks - 1],
            recv_sem=last_sem.at[h],
            device_id=(ds, dm),
            device_id_type=MESH,
        )

    def power_copy(ds, dm):
        return pltpu.make_async_remote_copy(
            src_ref=pw_send,
            dst_ref=pw_recv.at[me],
            send_sem=pw_sem.at[0],
            recv_sem=pw_sem.at[1],
            device_id=(ds, dm),
            device_id_type=MESH,
        )

    def whole(ref, first, second):
        return pltpu.make_async_remote_copy(
            src_ref=ref,
            dst_ref=ref,
            send_sem=first,
            recv_sem=second,
            device_id=(s, m),
            device_id_type=MESH,
        )

    others = pl.ds(0, (group - 1) * blk)

    def prepare(xp, total):
        field_copy(xp).wait()
        for q in range(2):
            value = jnp.concatenate([fld[q, 2 * xp], fld[q, 2 * xp + 1]], axis=1)
            high, low = split(value)
            fh[xp, pl.ds(q * ny, ny), :] = high
            fl[xp, pl.ds(q * ny, ny), :] = low
            total = total + jnp.sum((value * value).reshape(ny // 8, 8, 2 * cols), axis=0)
        return total

    def along_y(c, xp):
        result = left_table(fwd[c], fh[xp], fl[xp])
        turn[pl.ds(2 * xp * pitch, 2 * group), :] = result[:, :cols]
        turn[pl.ds((2 * xp + 1) * pitch, 2 * group), :] = result[:, cols:]

    def lay_out(c, h):
        for r in range(group):
            for q in range(2):
                send[c, pl.ds(r * blk + h * rows + q * 8, 8), :] = turn[
                    pl.ds(h * 8 * pitch + q * group + r, 8, stride=pitch), :
                ]
        for q in range(2):
            recv[c, pl.ds(me * blk + h * rows + q * 8, 8), :] = turn[
                pl.ds(h * 8 * pitch + q * group + me, 8, stride=pitch), :
            ]

    total = jnp.zeros((8, 2 * cols), jnp.float32)
    for h in range(2):
        for xp in range(h * pairs // 2, (h + 1) * pairs // 2):
            total = prepare(xp, total)
        if h == 0:
            tables[0].wait()
        else:
            for copy in tables[1:]:
                copy.start()
            tile = jnp.sum(total[:, :cols] + total[:, cols:], axis=0, keepdims=True)
            pw_send[...] = tile
            pw_recv[me] = tile
            to_all(lambda ds, dm: power_copy(ds, dm).start())
        for xp in range(h * pairs // 2, (h + 1) * pairs // 2):
            along_y(0, xp)
        lay_out(0, h)
        if h == 0:
            pl.semaphore_wait(barrier, group - 1)
        to_all(lambda ds, dm: forward_copy(0, ds, dm, h * rows, rows).start())
    tables[1].wait()

    def rest(c, carry):
        def body(xp, inner):
            along_y(c, xp)
            return inner

        lax.fori_loop(0, pairs, body, 0)
        for h in range(2):
            lay_out(c, h)
        to_all(lambda ds, dm: forward_copy(c, ds, dm, 0, blk).start())
        return carry

    lax.fori_loop(1, chunks, rest, 0)

    for copy in tables[2:]:
        copy.wait()
    other_tiles = pw_recv.at[pl.ds(0, group - 1)]
    whole(other_tiles, pw_sem.at[0], pw_sem.at[1]).wait_recv()
    power = jnp.sum(jnp.sum(pw_recv[...], axis=0), axis=(0, 1), keepdims=True)
    scale = 1.0 / jnp.sqrt(power / (nx * ny * nt) + EPSILON)
    place_x = place(lax.broadcasted_iota(jnp.int32, (nx, WIDE), 0), nx)
    square_x = place_x * place_x
    tiles = nt // WIDE
    per_tile = WIDE // cols

    def along_t(source, n):
        lanes = pl.ds(n * WIDE, WIDE)
        parts = []
        for part in range(2):
            both = dot(source[...], wt[part, 0, :, lanes])
            parts.append(
                both[: 2 * nx] + both[2 * nx :] + dot(source[: 2 * nx], wt[part, 1, :, lanes])
            )
        gr, gi = parts
        return gr[:nx] - gi[nx:], gi[:nx] + gr[nx:]

    def middle(c):
        whole(recv.at[c, others], send_sem.at[c], recv_sem.at[c]).wait_recv()
        for a in range(slabs):
            for b in range(times):
                for q in range(2):
                    row = (a * times + b) * blk + q * 8
                    got = jnp.concatenate(
                        [recv[c, pl.ds(row + h * rows, 8), :] for h in range(2)], axis=0
                    )
                    high, low = split(got)
                    xh[pl.ds(q * nx + a * rows, rows), pl.ds(b * cols, cols)] = high
                    xl[pl.ds(q * nx + a * rows, rows), pl.ds(b * cols, cols)] = low
        for n in range(tiles):
            lanes = pl.ds(n * WIDE, WIDE)
            value = left_table(across[...], xh[:, lanes], xl[:, lanes])
            high, low = split(value)
            ysp[pl.ds(0, 2 * nx), lanes] = high
            ysp[pl.ds(2 * nx, 2 * nx), lanes] = low
        y = c * group + me
        place_y = (y.astype(jnp.float32) - (ny - 1) / 2.0) / (ny / 2.0)
        well_depth = WELL * (square_x + place_y * place_y)
        for n in range(tiles):
            lanes = pl.ds(n * WIDE, WIDE)
            real, imag = along_t(ysp, n)
            real, imag = kick(real, imag, scale, well_depth)
            for q, value in enumerate((real, imag)):
                high, low = split(value)
                ksp[pl.ds(q * nx, nx), lanes] = high
                ksp[pl.ds((2 + q) * nx, nx), lanes] = low
        for n in range(tiles):
            lanes = pl.ds(n * WIDE, WIDE)
            for q, value in enumerate(along_t(ksp, n)):
                high, low = split(value)
                xh[pl.ds(q * nx, nx), lanes] = high
                xl[pl.ds(q * nx, nx), lanes] = low
        for n in range(tiles):
            lanes = pl.ds(n * WIDE, WIDE)
            value = left_table(across[...], xh[:, lanes], xl[:, lanes])
            for q in range(2):
                for a in range(slabs):
                    for b in range(per_tile):
                        dest = a * times + n * per_tile + b
                        for h in range(2):
                            first = q * nx + a * rows + h * 8
                            hsend[c, pl.ds(dest * blk + h * rows + q * 8, 8), :] = value[
                                first : first + 8, b * cols : (b + 1) * cols
                            ]

    def most(c, carry):
        middle(c)
        home[c, pl.ds(me * hpitch, blk), :] = hsend[c, pl.ds(me * blk, blk), :]
        to_all(lambda ds, dm: home_copy(c, ds, dm).start())
        return carry

    lax.fori_loop(0, chunks - 1, most, 0)
    middle(chunks - 1)
    home_last[pl.ds(me * hpitch, blk), :] = hsend[chunks - 1, pl.ds(me * blk, blk), :]
    for h in range(2):
        to_all(lambda ds, dm: last_copy(h, ds, dm).start())

    acc[...] = jnp.zeros_like(acc)

    def gather(c, carry):
        whole(home.at[c, others], hsend_sem.at[c], home_sem.at[c]).wait_recv()
        source = home.at[c]

        def add_up(xp, inner):
            start = (xp // 4) * rows + (2 * xp) % 8
            high, low = home_pair(source, start, hpitch, group, rows)
            value = stacked_table(back[c], high, low)
            for q in range(2):
                for i in range(2):
                    part = value[q * ny : (q + 1) * ny, i * cols : (i + 1) * cols]
                    acc[q, 2 * xp + i] = acc[q, 2 * xp + i] + part
            return inner

        lax.fori_loop(0, pairs, add_up, 0)
        return carry

    lax.fori_loop(0, chunks - 1, gather, 0)

    def drain(c, carry):
        whole(send.at[c, others], send_sem.at[c], recv_sem.at[c]).wait_send()
        whole(hsend.at[c, others], hsend_sem.at[c], home_sem.at[c]).wait_send()
        return carry

    lax.fori_loop(0, chunks - 1, drain, 0)
    whole(send.at[chunks - 1, others], send_sem.at[chunks - 1], recv_sem.at[chunks - 1]).wait_send()
    whole(other_tiles, pw_sem.at[0], pw_sem.at[1]).wait_send()

    half_others = pl.ds(0, (group - 1) * rows)
    whole(home_last.at[half_others], hsend_sem.at[chunks - 1], last_sem.at[0]).wait_recv()
    for xp in range(pairs // 2):
        start = (xp // 4) * rows + (2 * xp) % 8
        high, low = home_pair(home_last, start, hpitch, group, rows)
        value = stacked_table(back[chunks - 1], high, low)
        for q in range(2):
            for i in range(2):
                part = value[q * ny : (q + 1) * ny, i * cols : (i + 1) * cols]
                acc[q, 2 * xp + i] = acc[q, 2 * xp + i] + part
    whole(hsend.at[chunks - 1, others], hsend_sem.at[chunks - 1], last_sem.at[1]).wait_send()
    whole(home_last.at[half_others], hsend_sem.at[chunks - 1], last_sem.at[1]).wait_recv()


def finish_kernel(dims, acc, home_last, back, out_ref, stage, out_sem):
    group, rows, ny, cols = dims
    hpitch = home_last.shape[0] // group
    pairs = rows // 2

    def early(xp):
        part = (slice(None), pl.ds(2 * xp, 2))
        return pltpu.make_async_copy(acc.at[part], out_ref.at[part], out_sem.at[xp])

    def late(xp):
        return pltpu.make_async_copy(
            stage.at[:, pl.ds(2 * xp - rows // 2, 2)],
            out_ref.at[:, pl.ds(2 * xp, 2)],
            out_sem.at[xp],
        )

    for xp in range(pairs // 2):
        early(xp).start()
    for xp in range(pairs // 2, pairs):
        start = (xp // 4) * rows + (2 * xp) % 8
        high, low = home_pair(home_last, start, hpitch, group, rows)
        value = stacked_table(back[...], high, low)
        for q in range(2):
            for i in range(2):
                part = value[q * ny : (q + 1) * ny, i * cols : (i + 1) * cols]
                stage[q, 2 * xp - rows // 2 + i] = acc[q, 2 * xp + i] + part
        late(xp).start()
    for xp in range(pairs // 2):
        early(xp).wait()
    for xp in range(pairs // 2, pairs):
        late(xp).wait()


def in_kernels(field, slabs, times):
    _, rows, ny, cols = field.shape
    group = slabs * times
    nx, nt = rows * slabs, cols * times
    chunks = ny // group
    blk = 2 * rows
    hpitch = blk + 8
    pitch = 2 * group + 8
    uy = matrix(ny, -DIFFRACT)
    ux = matrix(nx, -DIFFRACT)
    ut = matrix(nt, DISPERSE)
    full_y = blocks(uy).reshape(2, ny, 2, ny)
    fwd, back = [], []
    for c in range(chunks):
        mine = slice(c * group, (c + 1) * group)
        fwd.append(np.concatenate(halves(full_y[:, mine].reshape(2 * group, 2 * ny))))
        high, low = halves(full_y[:, :, :, mine].reshape(2 * ny, 2 * group))
        back.append(np.concatenate([high, low, high], axis=1))
    fwd, back = np.stack(fwd), np.stack(back)
    across = np.concatenate(halves(blocks(ux)))
    time = np.stack([np.stack(halves(ut.real)), np.stack(halves(ut.imag))])
    dims = (slabs, times, rows, ny, cols, chunks)
    f32, bf16 = jnp.float32, jnp.bfloat16
    hbm = pl.BlockSpec(memory_space=pltpu.HBM)
    vmem = pl.BlockSpec(memory_space=pltpu.VMEM)
    dma = pltpu.SemaphoreType.DMA
    acc, home_last = pl.pallas_call(
        functools.partial(step_kernel, dims),
        out_shape=(
            jax.ShapeDtypeStruct(field.shape, f32),
            jax.ShapeDtypeStruct((group * hpitch, cols), f32),
        ),
        in_specs=[hbm] * 5,
        out_specs=(vmem, vmem),
        scratch_shapes=[
            pltpu.VMEM(field.shape, f32),
            pltpu.VMEM((rows // 2, 2 * ny, 2 * cols), bf16),
            pltpu.VMEM((rows // 2, 2 * ny, 2 * cols), bf16),
            pltpu.VMEM(fwd.shape, bf16),
            pltpu.VMEM(across.shape, bf16),
            pltpu.VMEM(time.shape, bf16),
            pltpu.VMEM(back.shape, bf16),
            pltpu.VMEM((rows * pitch, cols), f32),
            pltpu.VMEM((chunks, group * blk, cols), f32),
            pltpu.VMEM((chunks, group * blk, cols), f32),
            pltpu.VMEM((2 * nx, nt), bf16),
            pltpu.VMEM((2 * nx, nt), bf16),
            pltpu.VMEM((4 * nx, nt), bf16),
            pltpu.VMEM((4 * nx, nt), bf16),
            pltpu.VMEM((chunks, group * blk, cols), f32),
            pltpu.VMEM((chunks - 1, group * hpitch, cols), f32),
            pltpu.VMEM((1, cols), f32),
            pltpu.VMEM((group, 1, cols), f32),
            dma((rows // 2,)),
            dma((5,)),
            dma((chunks,)),
            dma((chunks,)),
            dma((chunks,)),
            dma((chunks - 1,)),
            dma((2,)),
            dma((2,)),
        ],
        compiler_params=pltpu.CompilerParams(
            collective_id=0, has_side_effects=True, vmem_limit_bytes=48 * 1024 * 1024
        ),
    )(field, *[pltpu.with_memory_space_constraint(jnp.asarray(a), pltpu.HBM) for a in (fwd, across, time, back)])
    return pl.pallas_call(
        functools.partial(finish_kernel, (group, rows, ny, cols)),
        out_shape=jax.ShapeDtypeStruct(field.shape, f32),
        in_specs=[vmem] * 3,
        out_specs=hbm,
        scratch_shapes=[
            pltpu.VMEM((2, rows // 2, ny, cols), f32),
            dma((rows // 2,)),
        ],
        compiler_params=pltpu.CompilerParams(vmem_limit_bytes=16 * 1024 * 1024),
    )(acc, home_last, jnp.asarray(back[-1]))


def on_device(field):
    slabs = lax.axis_size("slab")
    times = lax.axis_size("tm")
    devices = slabs * times
    _, rows, ny, cols = field.shape
    nx = rows * slabs
    nt = cols * times
    if (
        ny % devices == 0
        and ny // devices > 2
        and devices % 8 == 0
        and rows == 16
        and cols == LANES
        and nt % WIDE == 0
        and times % 2 == 0
    ):
        return in_kernels(field, slabs, times)

    along_x = propagator(nx, -DIFFRACT)
    along_y = propagator(ny, -DIFFRACT)
    along_t = propagator(nt, DISPERSE)
    partial_power = jnp.sum(field[0] * field[0] + field[1] * field[1])
    mean_power = lax.psum(partial_power, AXES) / (nx * ny * nt)
    scale = 1.0 / jnp.sqrt(mean_power + EPSILON)
    index_x = jnp.arange(nx, dtype=jnp.int32)
    group = ny // times
    width = group * nt // slabs
    sent = apply("qzpb,pabc->qazc", along_y, field)
    timed = lax.all_to_all(sent, "tm", split_axis=2, concat_axis=3, tiled=True)
    timed = apply("rtqT,qabT->rabt", along_t, timed)
    crossed = lax.all_to_all(
        timed.reshape(2, rows, slabs, width), "slab", split_axis=2, concat_axis=1, tiled=True
    ).reshape(2, nx, width)
    crossed = apply("qxpX,pXw->qxw", along_x, crossed)
    flat = lax.axis_index("slab") * width + jnp.arange(width, dtype=jnp.int32)
    place_y = place(lax.axis_index("tm") * group + flat // nt, ny)
    well_depth = WELL * (place(index_x, nx)[:, None] ** 2 + place_y[None, :] ** 2)
    kicked = jnp.stack(kick(crossed[0], crossed[1], scale, well_depth))
    kicked = apply("qxpX,pXw->qxw", along_x, kicked)
    timed = lax.all_to_all(
        kicked.reshape(2, nx, 1, width), "slab", split_axis=1, concat_axis=2, tiled=True
    ).reshape(2, rows, group, nt)
    timed = apply("rtqT,qabT->rabt", along_t, timed)
    home = lax.all_to_all(timed, "tm", split_axis=3, concat_axis=2, tiled=True)
    return apply("qzpb,pabc->qazc", along_y, home)


def solution(mesh):
    placed = (P(None, "slab", None, "tm"),)
    return jax.shard_map(
        on_device,
        mesh=mesh,
        in_specs=placed,
        out_specs=P(None, "slab", None, "tm"),
        check_vma=False,
    )
```

```python
import functools
import math

import ml_dtypes
import numpy as np

import jax
import jax.numpy as jnp
from jax import lax
from jax.experimental import pallas as pl
from jax.experimental.pallas import tpu as pltpu
from jax.sharding import PartitionSpec as P

TWO_PI = 2.0 * math.pi
DIFFRACT = 4.0
DISPERSE = 3.0
KERR = 0.05
WELL = 1.5
EPSILON = 1e-06
AXES = ("slab", "tm")
LANES = 128
WIDE = 256
MESH = pl.DeviceIdType.MESH


def matrix(length, strength):
    steps = np.arange(length)
    signed = np.where(2 * steps < length, steps, steps - length)
    phase = np.exp(1j * strength * (TWO_PI * signed / length) ** 2)
    response = np.fft.ifft(phase)
    return response[(steps[:, None] - steps[None, :]) % length]


def propagator(length, strength):
    whole = matrix(length, strength)
    real = jnp.asarray(whole.real.astype(np.float32))
    imag = jnp.asarray(whole.imag.astype(np.float32))
    upper = jnp.stack([real, -imag], axis=1)
    lower = jnp.stack([imag, real], axis=1)
    return jnp.stack([upper, lower])


def halves(table):
    table = table.astype(np.float32)
    high = table.astype(ml_dtypes.bfloat16)
    low = (table - high.astype(np.float32)).astype(ml_dtypes.bfloat16)
    return high, low


def blocks(whole):
    return np.block([[whole.real, -whole.imag], [whole.imag, whole.real]])


def apply(form, table, value):
    return jnp.einsum(form, table, value, precision=lax.Precision.HIGH)


def place(index, length):
    return (index.astype(jnp.float32) - (length - 1) / 2.0) / (length / 2.0)


def kick(real, imag, scale, well_depth):
    real = real * scale
    imag = imag * scale
    angle = KERR * (real * real + imag * imag) - well_depth
    turn_c = jnp.cos(angle)
    turn_s = jnp.sin(angle)
    return real * turn_c - imag * turn_s, real * turn_s + imag * turn_c


def split(value):
    high = value.astype(jnp.bfloat16)
    low = (value - high.astype(jnp.float32)).astype(jnp.bfloat16)
    return high, low


def dot(left, right):
    return jnp.dot(left, right, preferred_element_type=jnp.float32)


def left_table(table, high, low):
    n = table.shape[0] // 2
    both = dot(table, high)
    return both[:n] + both[n:] + dot(table[:n], low)


def stacked_table(table, high, low):
    return dot(table, jnp.concatenate([high, high, low], axis=0))


def home_pair(home, h, first, slabs, times):
    sides = []
    for i in range(2):
        pieces = []
        for q in range(2):
            for b in range(times):
                start = ((b * 2 + h) * slabs * 2 + q) * 8 + first + i
                pieces.append(home[pl.ds(start, slabs, stride=16), :])
        sides.append(jnp.concatenate(pieces, axis=0))
    return split(jnp.concatenate(sides, axis=1))


def step_kernel(
    dims,
    field_ref,
    fwd_ref,
    across_ref,
    time_ref,
    back_ref,
    acc,
    home,
    fld,
    fh,
    fl,
    fwd,
    across,
    wt,
    back,
    turn,
    zsend,
    zrecv,
    asend,
    arecv,
    bsend,
    brecv,
    hsend,
    ysp,
    pw_send,
    pw_recv,
    pw_all,
    load_sem,
    table_sem,
    zsend_sem,
    zrecv_sem,
    asend_sem,
    arecv_sem,
    bsend_sem,
    brecv_sem,
    hsend_sem,
    home_sem,
    pw_sem,
):
    slabs, times, rows, ny, cols, chunks = dims
    group = slabs * times
    nx, nt = slabs * rows, times * cols
    blk = 2 * rows
    zhalf = slabs * rows
    zblk = 2 * zhalf
    pitch = turn.shape[0] // rows
    pairs = rows // 2
    some = pairs // 2
    s = lax.axis_index("slab")
    m = lax.axis_index("tm")

    def field_copy(xp):
        part = (slice(None), pl.ds(2 * xp, 2))
        return pltpu.make_async_copy(field_ref.at[part], fld.at[part], load_sem.at[xp])

    rest_rows = pl.ds(1, chunks - 1)
    tables = [
        pltpu.make_async_copy(a, b, table_sem.at[i])
        for i, (a, b) in enumerate(
            [
                (fwd_ref.at[0], fwd.at[0]),
                (fwd_ref.at[rest_rows], fwd.at[rest_rows]),
                (across_ref, across),
                (time_ref, wt),
                (back_ref, back),
            ]
        )
    ]
    tables[0].start()
    for xp in range(pairs):
        field_copy(xp).start()

    half = times // 2
    side = m // half
    line = [(1 - side) * half + (m + i) % half for i in range(half)]
    line = line + [side * half + (m + i) % half for i in range(1, half)]
    ring = [(s + k) % slabs for k in range(1, slabs)]

    barrier = pltpu.get_barrier_semaphore()
    for there in line:
        pl.semaphore_signal(barrier, inc=1, device_id=(s, there), device_id_type=MESH)
    for there in ring:
        pl.semaphore_signal(barrier, inc=1, device_id=(there, m), device_id_type=MESH)

    def remote(src, dst, first, second, device):
        return pltpu.make_async_remote_copy(
            src_ref=src,
            dst_ref=dst,
            send_sem=first,
            recv_sem=second,
            device_id=device,
            device_id_type=MESH,
        )

    def whole(ref, first, second):
        return remote(ref, ref, first, second, (s, m))

    def out_along_t(c, h):
        for there in line:
            remote(
                zsend.at[c, pl.ds(there * zblk + h * zhalf, zhalf)],
                zrecv.at[c, pl.ds(m * zblk + h * zhalf, zhalf)],
                zsend_sem.at[c],
                zrecv_sem.at[c],
                (s, there),
            ).start()

    def out_across(c):
        for there in ring:
            remote(
                asend.at[c, pl.ds(there * blk, blk)],
                arecv.at[c, pl.ds(s * blk, blk)],
                asend_sem.at[c],
                arecv_sem.at[c],
                (there, m),
            ).start()

    def home_across(c):
        for there in ring:
            remote(
                bsend.at[c, pl.ds(there * blk, blk)],
                brecv.at[c, pl.ds(s * blk, blk)],
                bsend_sem.at[c],
                brecv_sem.at[c],
                (there, m),
            ).start()

    def home_along_t(c, h):
        for there in line:
            remote(
                hsend.at[c, pl.ds(there * zblk + h * zhalf, zhalf)],
                home.at[c, pl.ds(m * zblk + h * zhalf, zhalf)],
                hsend_sem.at[c],
                home_sem.at[c, h],
                (s, there),
            ).start()

    z_others = pl.ds(0, (times - 1) * zblk)
    z_half_others = pl.ds(0, (times - 1) * zhalf)
    a_others = pl.ds(0, (slabs - 1) * blk)

    def prepare(xp, total):
        field_copy(xp).wait()
        for q in range(2):
            value = jnp.concatenate([fld[q, 2 * xp], fld[q, 2 * xp + 1]], axis=1)
            high, low = split(value)
            fh[xp, pl.ds(q * ny, ny), :] = high
            fl[xp, pl.ds(q * ny, ny), :] = low
            total = total + jnp.sum((value * value).reshape(ny // 8, 8, 2 * cols), axis=0)
        return total

    def along_y(c, xp):
        result = left_table(fwd[c], fh[xp], fl[xp])
        turn[pl.ds(2 * xp * pitch, 2 * group), :] = result[:, :cols]
        turn[pl.ds((2 * xp + 1) * pitch, 2 * group), :] = result[:, cols:]

    def lay_out(c, h):
        for there in range(times):
            for k in range(slabs):
                for q in range(2):
                    zsend[c, pl.ds(there * zblk + h * zhalf + k * rows + q * 8, 8), :] = turn[
                        pl.ds(h * 8 * pitch + q * group + there * slabs + k, 8, stride=pitch), :
                    ]
        mine = pl.ds(m * zblk + h * zhalf, zhalf)
        zrecv[c, mine, :] = zsend[c, mine, :]

    total = jnp.zeros((8, 2 * cols), jnp.float32)
    for h in range(2):
        for xp in range(h * some, (h + 1) * some):
            total = prepare(xp, total)
        if h == 0:
            tables[0].wait()
        else:
            for copy in tables[1:]:
                copy.start()
            tile = jnp.sum(total[:, :cols] + total[:, cols:], axis=0, keepdims=True)
            pw_send[0] = tile
            pw_recv[s] = tile
            for there in ring:
                remote(
                    pw_send.at[0], pw_recv.at[s], pw_sem.at[0], pw_sem.at[1], (there, m)
                ).start()
        for xp in range(h * some, (h + 1) * some):
            along_y(0, xp)
        lay_out(0, h)
        if h == 0:
            pl.semaphore_wait(barrier, times - 1 + slabs - 1)
        out_along_t(0, h)
    slab_tiles = pw_recv.at[pl.ds(0, slabs - 1)]
    whole(slab_tiles, pw_sem.at[0], pw_sem.at[1]).wait_recv()
    tile = jnp.sum(pw_recv[...], axis=0)
    pw_send[1] = tile
    pw_all[m] = tile
    for there in line:
        remote(pw_send.at[1], pw_all.at[m], pw_sem.at[2], pw_sem.at[3], (s, there)).start()
    tables[1].wait()

    def rest(c, carry):
        def body(xp, inner):
            along_y(c, xp)
            return inner

        lax.fori_loop(0, pairs, body, 0)
        for h in range(2):
            lay_out(c, h)
            out_along_t(c, h)
        return carry

    lax.fori_loop(1, chunks, rest, 0)

    for copy in tables[2:]:
        copy.wait()
    line_tiles = pw_all.at[pl.ds(0, times - 1)]
    whole(line_tiles, pw_sem.at[2], pw_sem.at[3]).wait_recv()
    power = jnp.sum(jnp.sum(pw_all[...], axis=0), axis=(0, 1), keepdims=True)
    scale = 1.0 / jnp.sqrt(power / (nx * ny * nt) + EPSILON)
    sets = 2 * slabs
    position = lax.broadcasted_iota(jnp.int32, (sets, 8, WIDE), 0) * 8
    position = position + lax.broadcasted_iota(jnp.int32, (sets, 8, WIDE), 1)
    place_x = place(position, nx)
    square_x = place_x * place_x
    tiles = nt // WIDE
    per_tile = WIDE // cols

    def parts_of(value):
        value = value.reshape(sets, 2, 8, WIDE)
        return value[:, 0], value[:, 1]

    def along_t(n):
        lanes = pl.ds(n * WIDE, WIDE)
        products = []
        for part in range(2):
            both = dot(ysp[...], wt[part, 0, :, lanes])
            low = dot(ysp[: 2 * nx], wt[part, 1, :, lanes])
            products.append(parts_of(both[: 2 * nx] + both[2 * nx :] + low))
        (rr, ir), (ri, ii) = products
        return rr - ii, ri + ir

    def first_t(c):
        whole(zrecv.at[c, z_others], zsend_sem.at[c], zrecv_sem.at[c]).wait_recv()
        for b in range(times):
            high, low = split(zrecv[c, pl.ds(b * zblk, zblk), :])
            ysp[pl.ds(0, 2 * nx), pl.ds(b * cols, cols)] = high
            ysp[pl.ds(2 * nx, 2 * nx), pl.ds(b * cols, cols)] = low
        for n in range(tiles):
            lanes = pl.ds(n * WIDE, WIDE)
            for q, value in enumerate(along_t(n)):
                for h in range(2):
                    for k in range(slabs):
                        asend[c, pl.ds(k * blk + h * rows + q * 8, 8), lanes] = value[h * slabs + k]
        mine = pl.ds(s * blk, blk)
        arecv[c, mine, :] = asend[c, mine, :]
        out_across(c)

    def centre(c):
        whole(arecv.at[c, a_others], asend_sem.at[c], arecv_sem.at[c]).wait_recv()
        y = c * group + m * slabs + s
        place_y = (y.astype(jnp.float32) - (ny - 1) / 2.0) / (ny / 2.0)
        well_depth = WELL * (square_x + place_y * place_y)
        for n in range(tiles):
            lanes = pl.ds(n * WIDE, WIDE)
            real, imag = parts_of(left_table(across[...], *split(arecv[c, :, lanes])))
            real, imag = kick(real, imag, scale, well_depth)
            value = jnp.stack([real, imag], axis=1).reshape(2 * nx, WIDE)
            bsend[c, :, lanes] = left_table(across[...], *split(value))
        mine = pl.ds(s * blk, blk)
        brecv[c, mine, :] = bsend[c, mine, :]
        home_across(c)

    def second_t(c):
        whole(brecv.at[c, a_others], bsend_sem.at[c], brecv_sem.at[c]).wait_recv()
        high, low = split(brecv[c])
        ysp[pl.ds(0, 2 * nx), :] = high
        ysp[pl.ds(2 * nx, 2 * nx), :] = low
        for n in range(tiles):
            for q, value in enumerate(along_t(n)):
                for h in range(2):
                    for k in range(slabs):
                        for b in range(per_tile):
                            row = (n * per_tile + b) * zblk + h * zhalf + k * rows + q * 8
                            hsend[c, pl.ds(row, 8), :] = value[
                                k * 2 + h, :, b * cols : (b + 1) * cols
                            ]
        mine = pl.ds(m * zblk, zblk)
        home[c, mine, :] = hsend[c, mine, :]
        for h in range(2):
            home_along_t(c, h)

    def pipeline(i, carry):
        @pl.when(i < chunks)
        def _():
            first_t(i)

        @pl.when(jnp.logical_and(i >= 1, i < chunks + 1))
        def _():
            centre(i - 1)

        @pl.when(i >= 2)
        def _():
            second_t(i - 2)

        return carry

    lax.fori_loop(0, chunks + 2, pipeline, 0)

    acc[...] = jnp.zeros_like(acc)

    def add_up(c, source, h, xp, first):
        high, low = home_pair(source, h, first, slabs, times)
        value = stacked_table(back[c], high, low)
        for q in range(2):
            for i in range(2):
                part = value[q * ny : (q + 1) * ny, i * cols : (i + 1) * cols]
                acc[q, 2 * xp + i] = acc[q, 2 * xp + i] + part

    def gather(c, carry):
        source = home.at[c]
        for h in range(2):
            whole(home.at[c, z_half_others], hsend_sem.at[c], home_sem.at[c, h]).wait_recv()

            def body(k, inner):
                add_up(c, source, h, h * some + k, 2 * k)
                return inner

            lax.fori_loop(0, some, body, 0)
        return carry

    lax.fori_loop(0, chunks - 1, gather, 0)

    last = chunks - 1

    def drain(c, carry):
        whole(zsend.at[c, z_others], zsend_sem.at[c], zrecv_sem.at[c]).wait_send()
        whole(asend.at[c, a_others], asend_sem.at[c], arecv_sem.at[c]).wait_send()
        whole(bsend.at[c, a_others], bsend_sem.at[c], brecv_sem.at[c]).wait_send()
        return carry

    lax.fori_loop(0, chunks, drain, 0)
    whole(slab_tiles, pw_sem.at[0], pw_sem.at[1]).wait_send()
    whole(line_tiles, pw_sem.at[2], pw_sem.at[3]).wait_send()

    def drain_home(c, carry):
        whole(hsend.at[c, z_others], hsend_sem.at[c], home_sem.at[c, 0]).wait_send()
        return carry

    lax.fori_loop(0, last, drain_home, 0)
    whole(home.at[last, z_half_others], hsend_sem.at[last], home_sem.at[last, 0]).wait_recv()
    for xp in range(some):
        add_up(last, home.at[last], 0, xp, 2 * xp)
    drain_home(last, 0)
    whole(home.at[last, z_half_others], hsend_sem.at[last], home_sem.at[last, 1]).wait_recv()


def finish_kernel(dims, acc, home, back, out_ref, stage, out_sem):
    slabs, times, rows, ny, cols, chunks = dims
    pairs = rows // 2
    some = pairs // 2

    def early(xp):
        part = (slice(None), pl.ds(2 * xp, 2))
        return pltpu.make_async_copy(acc.at[part], out_ref.at[part], out_sem.at[xp])

    def late(k):
        return pltpu.make_async_copy(
            stage.at[:, pl.ds(2 * k, 2)],
            out_ref.at[:, pl.ds(rows // 2 + 2 * k, 2)],
            out_sem.at[some + k],
        )

    for xp in range(some):
        early(xp).start()
    for k in range(some):
        high, low = home_pair(home.at[chunks - 1], 1, 2 * k, slabs, times)
        value = stacked_table(back[...], high, low)
        for q in range(2):
            for i in range(2):
                part = value[q * ny : (q + 1) * ny, i * cols : (i + 1) * cols]
                stage[q, 2 * k + i] = acc[q, rows // 2 + 2 * k + i] + part
        late(k).start()
    for xp in range(some):
        early(xp).wait()
    for k in range(some):
        late(k).wait()


def in_kernels(field, slabs, times):
    _, rows, ny, cols = field.shape
    group = slabs * times
    nx, nt = rows * slabs, cols * times
    chunks = ny // group
    blk = 2 * rows
    pitch = 2 * group + 8
    uy = matrix(ny, -DIFFRACT)
    ux = matrix(nx, -DIFFRACT)
    ut = matrix(nt, DISPERSE)
    full_y = blocks(uy).reshape(2, ny, 2, ny)
    fwd, back = [], []
    for c in range(chunks):
        mine = slice(c * group, (c + 1) * group)
        fwd.append(np.concatenate(halves(full_y[:, mine].reshape(2 * group, 2 * ny))))
        high, low = halves(full_y[:, :, :, mine].reshape(2 * ny, 2 * group))
        back.append(np.concatenate([high, low, high], axis=1))
    fwd, back = np.stack(fwd), np.stack(back)
    full_x = blocks(ux).reshape(2, 2 * slabs, 8, 2, 2 * slabs, 8).transpose(1, 0, 2, 4, 3, 5)
    across = np.concatenate(halves(full_x.reshape(2 * nx, 2 * nx)))
    time = np.stack([np.stack(halves(ut.real)), np.stack(halves(ut.imag))])
    dims = (slabs, times, rows, ny, cols, chunks)
    f32, bf16 = jnp.float32, jnp.bfloat16
    hbm = pl.BlockSpec(memory_space=pltpu.HBM)
    vmem = pl.BlockSpec(memory_space=pltpu.VMEM)
    dma = pltpu.SemaphoreType.DMA
    narrow = (chunks, group * blk, cols)
    wide = (chunks, slabs * blk, nt)
    tables = [jnp.asarray(a) for a in (fwd, across, time, back)]
    acc, home = pl.pallas_call(
        functools.partial(step_kernel, dims),
        out_shape=(
            jax.ShapeDtypeStruct(field.shape, f32),
            jax.ShapeDtypeStruct(narrow, f32),
        ),
        in_specs=[hbm] * 5,
        out_specs=(vmem, vmem),
        scratch_shapes=[
            pltpu.VMEM(field.shape, f32),
            pltpu.VMEM((rows // 2, 2 * ny, 2 * cols), bf16),
            pltpu.VMEM((rows // 2, 2 * ny, 2 * cols), bf16),
            pltpu.VMEM(fwd.shape, bf16),
            pltpu.VMEM(across.shape, bf16),
            pltpu.VMEM(time.shape, bf16),
            pltpu.VMEM(back.shape, bf16),
            pltpu.VMEM((rows * pitch, cols), f32),
            pltpu.VMEM(narrow, f32),
            pltpu.VMEM(narrow, f32),
            pltpu.VMEM(wide, f32),
            pltpu.VMEM(wide, f32),
            pltpu.VMEM(wide, f32),
            pltpu.VMEM(wide, f32),
            pltpu.VMEM(narrow, f32),
            pltpu.VMEM((4 * nx, nt), bf16),
            pltpu.VMEM((2, 1, cols), f32),
            pltpu.VMEM((slabs, 1, cols), f32),
            pltpu.VMEM((times, 1, cols), f32),
            dma((rows // 2,)),
            dma((5,)),
            dma((chunks,)),
            dma((chunks,)),
            dma((chunks,)),
            dma((chunks,)),
            dma((chunks,)),
            dma((chunks,)),
            dma((chunks,)),
            dma((chunks, 2)),
            dma((4,)),
        ],
        compiler_params=pltpu.CompilerParams(
            collective_id=0, has_side_effects=True, vmem_limit_bytes=45 * 1024 * 1024
        ),
    )(field, *[pltpu.with_memory_space_constraint(a, pltpu.HBM) for a in tables])
    return pl.pallas_call(
        functools.partial(finish_kernel, dims),
        out_shape=jax.ShapeDtypeStruct(field.shape, f32),
        in_specs=[vmem] * 3,
        out_specs=hbm,
        scratch_shapes=[
            pltpu.VMEM((2, rows // 2, ny, cols), f32),
            dma((rows // 2,)),
        ],
        compiler_params=pltpu.CompilerParams(vmem_limit_bytes=16 * 1024 * 1024),
    )(acc, home, jnp.asarray(back[-1]))


def on_device(field):
    slabs = lax.axis_size("slab")
    times = lax.axis_size("tm")
    devices = slabs * times
    _, rows, ny, cols = field.shape
    nx = rows * slabs
    nt = cols * times
    if (
        ny % devices == 0
        and ny // devices > 2
        and slabs == 8
        and rows == 16
        and cols == LANES
        and nt % WIDE == 0
        and times % 2 == 0
    ):
        return in_kernels(field, slabs, times)

    along_x = propagator(nx, -DIFFRACT)
    along_y = propagator(ny, -DIFFRACT)
    along_t = propagator(nt, DISPERSE)
    partial_power = jnp.sum(field[0] * field[0] + field[1] * field[1])
    mean_power = lax.psum(partial_power, AXES) / (nx * ny * nt)
    scale = 1.0 / jnp.sqrt(mean_power + EPSILON)
    index_x = jnp.arange(nx, dtype=jnp.int32)
    group = ny // times
    width = group * nt // slabs
    sent = apply("qzpb,pabc->qazc", along_y, field)
    timed = lax.all_to_all(sent, "tm", split_axis=2, concat_axis=3, tiled=True)
    timed = apply("rtqT,qabT->rabt", along_t, timed)
    crossed = lax.all_to_all(
        timed.reshape(2, rows, slabs, width), "slab", split_axis=2, concat_axis=1, tiled=True
    ).reshape(2, nx, width)
    crossed = apply("qxpX,pXw->qxw", along_x, crossed)
    flat = lax.axis_index("slab") * width + jnp.arange(width, dtype=jnp.int32)
    place_y = place(lax.axis_index("tm") * group + flat // nt, ny)
    well_depth = WELL * (place(index_x, nx)[:, None] ** 2 + place_y[None, :] ** 2)
    kicked = jnp.stack(kick(crossed[0], crossed[1], scale, well_depth))
    kicked = apply("qxpX,pXw->qxw", along_x, kicked)
    timed = lax.all_to_all(
        kicked.reshape(2, nx, 1, width), "slab", split_axis=1, concat_axis=2, tiled=True
    ).reshape(2, rows, group, nt)
    timed = apply("rtqT,qabT->rabt", along_t, timed)
    home = lax.all_to_all(timed, "tm", split_axis=3, concat_axis=2, tiled=True)
    return apply("qzpb,pabc->qazc", along_y, home)


def solution(mesh):
    placed = (P(None, "slab", None, "tm"),)
    return jax.shard_map(
        on_device,
        mesh=mesh,
        in_specs=placed,
        out_specs=P(None, "slab", None, "tm"),
        check_vma=False,
    )
```

```python
import functools
import math

import ml_dtypes
import numpy as np

import jax
import jax.numpy as jnp
from jax import lax
from jax.experimental import pallas as pl
from jax.experimental.pallas import tpu as pltpu
from jax.sharding import PartitionSpec as P

TWO_PI = 2.0 * math.pi
DIFFRACT = 4.0
DISPERSE = 3.0
KERR = 0.05
WELL = 1.5
EPSILON = 1e-06
AXES = ("slab", "tm")
LANES = 128
WIDE = 256
MESH = pl.DeviceIdType.MESH


def matrix(length, strength):
    steps = np.arange(length)
    signed = np.where(2 * steps < length, steps, steps - length)
    phase = np.exp(1j * strength * (TWO_PI * signed / length) ** 2)
    response = np.fft.ifft(phase)
    return response[(steps[:, None] - steps[None, :]) % length]


def propagator(length, strength):
    whole = matrix(length, strength)
    real = jnp.asarray(whole.real.astype(np.float32))
    imag = jnp.asarray(whole.imag.astype(np.float32))
    upper = jnp.stack([real, -imag], axis=1)
    lower = jnp.stack([imag, real], axis=1)
    return jnp.stack([upper, lower])


def halves(table):
    table = table.astype(np.float32)
    high = table.astype(ml_dtypes.bfloat16)
    low = (table - high.astype(np.float32)).astype(ml_dtypes.bfloat16)
    return high, low


def blocks(whole):
    return np.block([[whole.real, -whole.imag], [whole.imag, whole.real]])


def apply(form, table, value):
    return jnp.einsum(form, table, value, precision=lax.Precision.HIGH)


def place(index, length):
    return (index.astype(jnp.float32) - (length - 1) / 2.0) / (length / 2.0)


def kick(real, imag, scale, well_depth):
    real = real * scale
    imag = imag * scale
    angle = KERR * (real * real + imag * imag) - well_depth
    turn_c = jnp.cos(angle)
    turn_s = jnp.sin(angle)
    return real * turn_c - imag * turn_s, real * turn_s + imag * turn_c


def split(value):
    high = value.astype(jnp.bfloat16)
    low = (value - high.astype(jnp.float32)).astype(jnp.bfloat16)
    return high, low


def dot(left, right):
    return jnp.dot(left, right, preferred_element_type=jnp.float32)


def left_table(table, high, low):
    n = table.shape[0] // 2
    both = dot(table, high)
    return both[:n] + both[n:] + dot(table[:n], low)


def stacked_table(table, high, low):
    return dot(table, jnp.concatenate([high, high, low], axis=0))


def home_pair(home, h, first, slabs, times):
    sides = []
    for i in range(2):
        pieces = []
        for q in range(2):
            for b in range(times):
                start = ((b * 2 + h) * slabs * 2 + q) * 8 + first + i
                pieces.append(home[pl.ds(start, slabs, stride=16), :])
        sides.append(jnp.concatenate(pieces, axis=0))
    return split(jnp.concatenate(sides, axis=1))


def step_kernel(
    dims,
    field_ref,
    fwd_ref,
    across_ref,
    time_ref,
    back_ref,
    acc,
    home,
    fld,
    fh,
    fl,
    fwd,
    across,
    wt,
    back,
    turn,
    zsend,
    zrecv,
    asend,
    arecv,
    bsend,
    brecv,
    hsend,
    ysp,
    pw_send,
    pw_recv,
    pw_all,
    load_sem,
    table_sem,
    zsend_sem,
    zrecv_sem,
    asend_sem,
    arecv_sem,
    bsend_sem,
    brecv_sem,
    hsend_sem,
    home_sem,
    pw_sem,
):
    slabs, times, rows, ny, cols, chunks = dims
    group = slabs * times
    nx, nt = slabs * rows, times * cols
    blk = 2 * rows
    zhalf = slabs * rows
    zblk = 2 * zhalf
    pitch = turn.shape[0] // rows
    pairs = rows // 2
    some = pairs // 2
    s = lax.axis_index("slab")
    m = lax.axis_index("tm")

    def field_copy(xp):
        part = (slice(None), pl.ds(2 * xp, 2))
        return pltpu.make_async_copy(field_ref.at[part], fld.at[part], load_sem.at[xp])

    rest_rows = pl.ds(1, chunks - 1)
    tables = [
        pltpu.make_async_copy(a, b, table_sem.at[i])
        for i, (a, b) in enumerate(
            [
                (fwd_ref.at[0], fwd.at[0]),
                (fwd_ref.at[rest_rows], fwd.at[rest_rows]),
                (across_ref, across),
                (time_ref, wt),
                (back_ref, back),
            ]
        )
    ]
    tables[0].start()
    for xp in range(some):
        field_copy(xp).start()

    half = times // 2
    side = m // half
    cross = [(1 - side) * half + i for i in range(half)]
    near = [side * half + (m + i) % half for i in range(1, half)]
    line = cross + near
    line_home = cross[:1] + near + cross[1:]
    ring = [(s + k) % slabs for k in range(1, slabs)]

    barrier = pltpu.get_barrier_semaphore()
    for there in line:
        pl.semaphore_signal(barrier, inc=1, device_id=(s, there), device_id_type=MESH)
    for there in ring:
        pl.semaphore_signal(barrier, inc=1, device_id=(there, m), device_id_type=MESH)

    def remote(src, dst, first, second, device):
        return pltpu.make_async_remote_copy(
            src_ref=src,
            dst_ref=dst,
            send_sem=first,
            recv_sem=second,
            device_id=device,
            device_id_type=MESH,
        )

    def whole(ref, first, second):
        return remote(ref, ref, first, second, (s, m))

    def out_along_t(c, first, count):
        for there in line:
            remote(
                zsend.at[c, pl.ds(there * zblk + first, count)],
                zrecv.at[c, pl.ds(m * zblk + first, count)],
                zsend_sem.at[c],
                zrecv_sem.at[c],
                (s, there),
            ).start()

    def out_across(c):
        for there in ring:
            remote(
                asend.at[c, pl.ds(there * blk, blk)],
                arecv.at[c, pl.ds(s * blk, blk)],
                asend_sem.at[c],
                arecv_sem.at[c],
                (there, m),
            ).start()

    def home_across(c):
        for there in ring:
            remote(
                bsend.at[c, pl.ds(there * blk, blk)],
                brecv.at[c, pl.ds(s * blk, blk)],
                bsend_sem.at[c],
                brecv_sem.at[c],
                (there, m),
            ).start()

    def home_along_t(c, there, first, count, arrived):
        remote(
            hsend.at[c, pl.ds(there * zblk + first, count)],
            home.at[c, pl.ds(m * zblk + first, count)],
            hsend_sem.at[c],
            arrived,
            (s, there),
        ).start()

    z_others = pl.ds(0, (times - 1) * zblk)
    z_half_others = pl.ds(0, (times - 1) * zhalf)
    a_others = pl.ds(0, (slabs - 1) * blk)

    def prepare(xp, total):
        field_copy(xp).wait()
        for q in range(2):
            value = jnp.concatenate([fld[q, 2 * xp], fld[q, 2 * xp + 1]], axis=1)
            high, low = split(value)
            fh[xp, pl.ds(q * ny, ny), :] = high
            fl[xp, pl.ds(q * ny, ny), :] = low
            total = total + jnp.sum((value * value).reshape(ny // 8, 8, 2 * cols), axis=0)
        return total

    def along_y(c, xp):
        result = left_table(fwd[c], fh[xp], fl[xp])
        turn[pl.ds(2 * xp * pitch, 2 * group), :] = result[:, :cols]
        turn[pl.ds((2 * xp + 1) * pitch, 2 * group), :] = result[:, cols:]

    def lay_out(c, h):
        for there in range(times):
            for k in range(slabs):
                for q in range(2):
                    zsend[c, pl.ds(there * zblk + h * zhalf + k * rows + q * 8, 8), :] = turn[
                        pl.ds(h * 8 * pitch + q * group + there * slabs + k, 8, stride=pitch), :
                    ]
        mine = pl.ds(m * zblk + h * zhalf, zhalf)
        zrecv[c, mine, :] = zsend[c, mine, :]

    total = jnp.zeros((8, 2 * cols), jnp.float32)
    for h in range(2):
        for xp in range(h * some, (h + 1) * some):
            total = prepare(xp, total)
            if xp < some:
                field_copy(some + xp).start()
        if h == 0:
            tables[0].wait()
        else:
            for copy in tables[1:]:
                copy.start()
            tile = jnp.sum(total[:, :cols] + total[:, cols:], axis=0, keepdims=True)
            pw_send[0] = tile
            pw_recv[s] = tile
            for there in ring:
                remote(
                    pw_send.at[0], pw_recv.at[s], pw_sem.at[0], pw_sem.at[1], (there, m)
                ).start()
        for xp in range(h * some, (h + 1) * some):
            along_y(0, xp)
        lay_out(0, h)
        if h == 0:
            pl.semaphore_wait(barrier, times - 1 + slabs - 1)
        out_along_t(0, h * zhalf, zhalf)
    slab_tiles = pw_recv.at[pl.ds(0, slabs - 1)]
    whole(slab_tiles, pw_sem.at[0], pw_sem.at[1]).wait_recv()
    tile = jnp.sum(pw_recv[...], axis=0)
    pw_send[1] = tile
    pw_all[m] = tile
    for there in line:
        remote(pw_send.at[1], pw_all.at[m], pw_sem.at[2], pw_sem.at[3], (s, there)).start()
    tables[1].wait()

    def rest(c, carry):
        def body(xp, inner):
            along_y(c, xp)
            return inner

        lax.fori_loop(0, pairs, body, 0)
        for h in range(2):
            lay_out(c, h)
        out_along_t(c, 0, zblk)
        return carry

    lax.fori_loop(1, chunks, rest, 0)

    for copy in tables[2:]:
        copy.wait()
    line_tiles = pw_all.at[pl.ds(0, times - 1)]
    whole(line_tiles, pw_sem.at[2], pw_sem.at[3]).wait_recv()
    power = jnp.sum(jnp.sum(pw_all[...], axis=0), axis=(0, 1), keepdims=True)
    scale = 1.0 / jnp.sqrt(power / (nx * ny * nt) + EPSILON)
    sets = 2 * slabs
    position = lax.broadcasted_iota(jnp.int32, (sets, 8, WIDE), 0) * 8
    position = position + lax.broadcasted_iota(jnp.int32, (sets, 8, WIDE), 1)
    place_x = place(position, nx)
    square_x = place_x * place_x
    tiles = nt // WIDE
    per_tile = WIDE // cols

    def parts_of(value):
        value = value.reshape(sets, 2, 8, WIDE)
        return value[:, 0], value[:, 1]

    def along_t(n):
        lanes = pl.ds(n * WIDE, WIDE)
        products = []
        for part in range(2):
            both = dot(ysp[...], wt[part, 0, :, lanes])
            low = dot(ysp[: 2 * nx], wt[part, 1, :, lanes])
            products.append(parts_of(both[: 2 * nx] + both[2 * nx :] + low))
        (rr, ir), (ri, ii) = products
        return rr - ii, ri + ir

    def first_t(c):
        whole(zrecv.at[c, z_others], zsend_sem.at[c], zrecv_sem.at[c]).wait_recv()
        for b in range(times):
            high, low = split(zrecv[c, pl.ds(b * zblk, zblk), :])
            ysp[pl.ds(0, 2 * nx), pl.ds(b * cols, cols)] = high
            ysp[pl.ds(2 * nx, 2 * nx), pl.ds(b * cols, cols)] = low
        for n in range(tiles):
            lanes = pl.ds(n * WIDE, WIDE)
            for q, value in enumerate(along_t(n)):
                for h in range(2):
                    for k in range(slabs):
                        asend[c, pl.ds(k * blk + h * rows + q * 8, 8), lanes] = value[h * slabs + k]
        mine = pl.ds(s * blk, blk)
        arecv[c, mine, :] = asend[c, mine, :]
        out_across(c)

    def centre(c):
        whole(arecv.at[c, a_others], asend_sem.at[c], arecv_sem.at[c]).wait_recv()
        y = c * group + m * slabs + s
        place_y = (y.astype(jnp.float32) - (ny - 1) / 2.0) / (ny / 2.0)
        well_depth = WELL * (square_x + place_y * place_y)
        for n in range(tiles):
            lanes = pl.ds(n * WIDE, WIDE)
            real, imag = parts_of(left_table(across[...], *split(arecv[c, :, lanes])))
            real, imag = kick(real, imag, scale, well_depth)
            value = jnp.stack([real, imag], axis=1).reshape(2 * nx, WIDE)
            bsend[c, :, lanes] = left_table(across[...], *split(value))
        mine = pl.ds(s * blk, blk)
        brecv[c, mine, :] = bsend[c, mine, :]
        home_across(c)

    def second_t(c):
        whole(brecv.at[c, a_others], bsend_sem.at[c], brecv_sem.at[c]).wait_recv()
        high, low = split(brecv[c])
        ysp[pl.ds(0, 2 * nx), :] = high
        ysp[pl.ds(2 * nx, 2 * nx), :] = low
        for n in range(tiles):
            for q, value in enumerate(along_t(n)):
                for h in range(2):
                    for k in range(slabs):
                        for b in range(per_tile):
                            row = (n * per_tile + b) * zblk + h * zhalf + k * rows + q * 8
                            hsend[c, pl.ds(row, 8), :] = value[
                                k * 2 + h, :, b * cols : (b + 1) * cols
                            ]
        mine = pl.ds(m * zblk, zblk)
        home[c, mine, :] = hsend[c, mine, :]

        @pl.when(c < chunks - 1)
        def _():
            for there in line_home:
                home_along_t(c, there, 0, zblk, home_sem.at[c])

        @pl.when(c == chunks - 1)
        def _():
            for there in line_home:
                for h in range(2):
                    home_along_t(c, there, h * zhalf, zhalf, home_sem.at[c + h])

    def pipeline(i, carry):
        @pl.when(i < chunks)
        def _():
            first_t(i)

        @pl.when(jnp.logical_and(i >= 1, i < chunks + 1))
        def _():
            centre(i - 1)

        @pl.when(i >= 2)
        def _():
            second_t(i - 2)

        return carry

    lax.fori_loop(0, chunks + 2, pipeline, 0)

    acc[...] = jnp.zeros_like(acc)

    def add_up(c, source, h, xp, first):
        high, low = home_pair(source, h, first, slabs, times)
        value = stacked_table(back[c], high, low)
        for q in range(2):
            for i in range(2):
                part = value[q * ny : (q + 1) * ny, i * cols : (i + 1) * cols]
                acc[q, 2 * xp + i] = acc[q, 2 * xp + i] + part

    def gather(c, carry):
        source = home.at[c]
        whole(home.at[c, z_others], hsend_sem.at[c], home_sem.at[c]).wait_recv()
        for h in range(2):

            def body(k, inner):
                add_up(c, source, h, h * some + k, 2 * k)
                return inner

            lax.fori_loop(0, some, body, 0)
        return carry

    lax.fori_loop(0, chunks - 1, gather, 0)

    last = chunks - 1

    def drain(c, carry):
        whole(zsend.at[c, z_others], zsend_sem.at[c], zrecv_sem.at[c]).wait_send()
        whole(asend.at[c, a_others], asend_sem.at[c], arecv_sem.at[c]).wait_send()
        whole(bsend.at[c, a_others], bsend_sem.at[c], brecv_sem.at[c]).wait_send()
        return carry

    lax.fori_loop(0, chunks, drain, 0)
    whole(slab_tiles, pw_sem.at[0], pw_sem.at[1]).wait_send()
    whole(line_tiles, pw_sem.at[2], pw_sem.at[3]).wait_send()

    def drain_home(c, carry):
        whole(hsend.at[c, z_others], hsend_sem.at[c], home_sem.at[c]).wait_send()
        return carry

    lax.fori_loop(0, last, drain_home, 0)
    whole(home.at[last, z_half_others], hsend_sem.at[last], home_sem.at[last]).wait_recv()
    for xp in range(some):
        add_up(last, home.at[last], 0, xp, 2 * xp)
    drain_home(last, 0)
    whole(home.at[last, z_half_others], hsend_sem.at[last], home_sem.at[last + 1]).wait_recv()


def finish_kernel(dims, acc, home, back, out_ref, stage, out_sem):
    slabs, times, rows, ny, cols, chunks = dims
    pairs = rows // 2
    some = pairs // 2

    def early(xp):
        part = (slice(None), pl.ds(2 * xp, 2))
        return pltpu.make_async_copy(acc.at[part], out_ref.at[part], out_sem.at[xp])

    def late(k):
        return pltpu.make_async_copy(
            stage.at[:, pl.ds(2 * k, 2)],
            out_ref.at[:, pl.ds(rows // 2 + 2 * k, 2)],
            out_sem.at[some + k],
        )

    for xp in range(some):
        early(xp).start()
    for k in range(some):
        high, low = home_pair(home.at[chunks - 1], 1, 2 * k, slabs, times)
        value = stacked_table(back[...], high, low)
        for q in range(2):
            for i in range(2):
                part = value[q * ny : (q + 1) * ny, i * cols : (i + 1) * cols]
                stage[q, 2 * k + i] = acc[q, rows // 2 + 2 * k + i] + part
        late(k).start()
    for xp in range(some):
        early(xp).wait()
    for k in range(some):
        late(k).wait()


def in_kernels(field, slabs, times):
    _, rows, ny, cols = field.shape
    group = slabs * times
    nx, nt = rows * slabs, cols * times
    chunks = ny // group
    blk = 2 * rows
    pitch = 2 * group + 8
    uy = matrix(ny, -DIFFRACT)
    ux = matrix(nx, -DIFFRACT)
    ut = matrix(nt, DISPERSE)
    full_y = blocks(uy).reshape(2, ny, 2, ny)
    fwd, back = [], []
    for c in range(chunks):
        mine = slice(c * group, (c + 1) * group)
        fwd.append(np.concatenate(halves(full_y[:, mine].reshape(2 * group, 2 * ny))))
        high, low = halves(full_y[:, :, :, mine].reshape(2 * ny, 2 * group))
        back.append(np.concatenate([high, low, high], axis=1))
    fwd, back = np.stack(fwd), np.stack(back)
    full_x = blocks(ux).reshape(2, 2 * slabs, 8, 2, 2 * slabs, 8).transpose(1, 0, 2, 4, 3, 5)
    across = np.concatenate(halves(full_x.reshape(2 * nx, 2 * nx)))
    time = np.stack([np.stack(halves(ut.real)), np.stack(halves(ut.imag))])
    dims = (slabs, times, rows, ny, cols, chunks)
    f32, bf16 = jnp.float32, jnp.bfloat16
    hbm = pl.BlockSpec(memory_space=pltpu.HBM)
    vmem = pl.BlockSpec(memory_space=pltpu.VMEM)
    dma = pltpu.SemaphoreType.DMA
    narrow = (chunks, group * blk, cols)
    wide = (chunks, slabs * blk, nt)
    tables = [jnp.asarray(a) for a in (fwd, across, time, back)]
    acc, home = pl.pallas_call(
        functools.partial(step_kernel, dims),
        out_shape=(
            jax.ShapeDtypeStruct(field.shape, f32),
            jax.ShapeDtypeStruct(narrow, f32),
        ),
        in_specs=[hbm] * 5,
        out_specs=(vmem, vmem),
        scratch_shapes=[
            pltpu.VMEM(field.shape, f32),
            pltpu.VMEM((rows // 2, 2 * ny, 2 * cols), bf16),
            pltpu.VMEM((rows // 2, 2 * ny, 2 * cols), bf16),
            pltpu.VMEM(fwd.shape, bf16),
            pltpu.VMEM(across.shape, bf16),
            pltpu.VMEM(time.shape, bf16),
            pltpu.VMEM(back.shape, bf16),
            pltpu.VMEM((rows * pitch, cols), f32),
            pltpu.VMEM(narrow, f32),
            pltpu.VMEM(narrow, f32),
            pltpu.VMEM(wide, f32),
            pltpu.VMEM(wide, f32),
            pltpu.VMEM(wide, f32),
            pltpu.VMEM(wide, f32),
            pltpu.VMEM(narrow, f32),
            pltpu.VMEM((4 * nx, nt), bf16),
            pltpu.VMEM((2, 1, cols), f32),
            pltpu.VMEM((slabs, 1, cols), f32),
            pltpu.VMEM((times, 1, cols), f32),
            dma((rows // 2,)),
            dma((5,)),
            dma((chunks,)),
            dma((chunks,)),
            dma((chunks,)),
            dma((chunks,)),
            dma((chunks,)),
            dma((chunks,)),
            dma((chunks,)),
            dma((chunks + 1,)),
            dma((4,)),
        ],
        compiler_params=pltpu.CompilerParams(
            collective_id=0, has_side_effects=True, vmem_limit_bytes=45 * 1024 * 1024
        ),
    )(field, *[pltpu.with_memory_space_constraint(a, pltpu.HBM) for a in tables])
    return pl.pallas_call(
        functools.partial(finish_kernel, dims),
        out_shape=jax.ShapeDtypeStruct(field.shape, f32),
        in_specs=[vmem] * 3,
        out_specs=hbm,
        scratch_shapes=[
            pltpu.VMEM((2, rows // 2, ny, cols), f32),
            dma((rows // 2,)),
        ],
        compiler_params=pltpu.CompilerParams(vmem_limit_bytes=16 * 1024 * 1024),
    )(acc, home, jnp.asarray(back[-1]))


def on_device(field):
    slabs = lax.axis_size("slab")
    times = lax.axis_size("tm")
    devices = slabs * times
    _, rows, ny, cols = field.shape
    nx = rows * slabs
    nt = cols * times
    if (
        ny % devices == 0
        and ny // devices > 2
        and slabs == 8
        and rows == 16
        and cols == LANES
        and nt % WIDE == 0
        and times % 2 == 0
    ):
        return in_kernels(field, slabs, times)

    along_x = propagator(nx, -DIFFRACT)
    along_y = propagator(ny, -DIFFRACT)
    along_t = propagator(nt, DISPERSE)
    partial_power = jnp.sum(field[0] * field[0] + field[1] * field[1])
    mean_power = lax.psum(partial_power, AXES) / (nx * ny * nt)
    scale = 1.0 / jnp.sqrt(mean_power + EPSILON)
    index_x = jnp.arange(nx, dtype=jnp.int32)
    group = ny // times
    width = group * nt // slabs
    sent = apply("qzpb,pabc->qazc", along_y, field)
    timed = lax.all_to_all(sent, "tm", split_axis=2, concat_axis=3, tiled=True)
    timed = apply("rtqT,qabT->rabt", along_t, timed)
    crossed = lax.all_to_all(
        timed.reshape(2, rows, slabs, width), "slab", split_axis=2, concat_axis=1, tiled=True
    ).reshape(2, nx, width)
    crossed = apply("qxpX,pXw->qxw", along_x, crossed)
    flat = lax.axis_index("slab") * width + jnp.arange(width, dtype=jnp.int32)
    place_y = place(lax.axis_index("tm") * group + flat // nt, ny)
    well_depth = WELL * (place(index_x, nx)[:, None] ** 2 + place_y[None, :] ** 2)
    kicked = jnp.stack(kick(crossed[0], crossed[1], scale, well_depth))
    kicked = apply("qxpX,pXw->qxw", along_x, kicked)
    timed = lax.all_to_all(
        kicked.reshape(2, nx, 1, width), "slab", split_axis=1, concat_axis=2, tiled=True
    ).reshape(2, rows, group, nt)
    timed = apply("rtqT,qabT->rabt", along_t, timed)
    home = lax.all_to_all(timed, "tm", split_axis=3, concat_axis=2, tiled=True)
    return apply("qzpb,pabc->qazc", along_y, home)


def solution(mesh):
    placed = (P(None, "slab", None, "tm"),)
    return jax.shard_map(
        on_device,
        mesh=mesh,
        in_specs=placed,
        out_specs=P(None, "slab", None, "tm"),
        check_vma=False,
    )
```

```python
import functools
import math

import ml_dtypes
import numpy as np

import jax
import jax.numpy as jnp
from jax import lax
from jax.experimental import pallas as pl
from jax.experimental.pallas import tpu as pltpu
from jax.sharding import PartitionSpec as P

TWO_PI = 2.0 * math.pi
DIFFRACT = 4.0
DISPERSE = 3.0
KERR = 0.05
WELL = 1.5
EPSILON = 1e-06
AXES = ("slab", "tm")
LANES = 128
WIDE = 256
MESH = pl.DeviceIdType.MESH


def matrix(length, strength):
    steps = np.arange(length)
    signed = np.where(2 * steps < length, steps, steps - length)
    phase = np.exp(1j * strength * (TWO_PI * signed / length) ** 2)
    response = np.fft.ifft(phase)
    return response[(steps[:, None] - steps[None, :]) % length]


def propagator(length, strength):
    whole = matrix(length, strength)
    real = jnp.asarray(whole.real.astype(np.float32))
    imag = jnp.asarray(whole.imag.astype(np.float32))
    upper = jnp.stack([real, -imag], axis=1)
    lower = jnp.stack([imag, real], axis=1)
    return jnp.stack([upper, lower])


def halves(table):
    table = table.astype(np.float32)
    high = table.astype(ml_dtypes.bfloat16)
    low = (table - high.astype(np.float32)).astype(ml_dtypes.bfloat16)
    return high, low


def blocks(whole):
    return np.block([[whole.real, -whole.imag], [whole.imag, whole.real]])


def apply(form, table, value):
    return jnp.einsum(form, table, value, precision=lax.Precision.HIGH)


def place(index, length):
    return (index.astype(jnp.float32) - (length - 1) / 2.0) / (length / 2.0)


def kick(real, imag, scale, well_depth):
    real = real * scale
    imag = imag * scale
    angle = KERR * (real * real + imag * imag) - well_depth
    turn_c = jnp.cos(angle)
    turn_s = jnp.sin(angle)
    return real * turn_c - imag * turn_s, real * turn_s + imag * turn_c


def split(value):
    high = value.astype(jnp.bfloat16)
    low = (value - high.astype(jnp.float32)).astype(jnp.bfloat16)
    return high, low


def dot(left, right):
    return jnp.dot(left, right, preferred_element_type=jnp.float32)


def left_table(table, high, low):
    n = table.shape[0] // 2
    both = dot(table, high)
    return both[:n] + both[n:] + dot(table[:n], low)


def stacked_table(table, high, low):
    return dot(table, jnp.concatenate([high, high, low], axis=0))


def home_pair(home, h, first, slabs, times):
    sides = []
    for i in range(2):
        pieces = []
        for q in range(2):
            for b in range(times):
                start = ((b * 2 + h) * slabs * 2 + q) * 8 + first + i
                pieces.append(home[pl.ds(start, slabs, stride=16), :])
        sides.append(jnp.concatenate(pieces, axis=0))
    return split(jnp.concatenate(sides, axis=1))


def step_kernel(
    dims,
    field_ref,
    fwd_ref,
    across_ref,
    time_ref,
    back_ref,
    acc,
    home,
    fld,
    fh,
    fl,
    fwd,
    across,
    wt,
    back,
    turn,
    zsend,
    zrecv,
    asend,
    arecv,
    bsend,
    brecv,
    hsend,
    ysp,
    pw_send,
    pw_recv,
    pw_all,
    load_sem,
    table_sem,
    zsend_sem,
    zrecv_sem,
    asend_sem,
    arecv_sem,
    bsend_sem,
    brecv_sem,
    hsend_sem,
    home_sem,
    pw_sem,
    line_ready,
    ring_ready,
):
    slabs, times, rows, ny, cols, chunks = dims
    group = slabs * times
    nx, nt = slabs * rows, times * cols
    blk = 2 * rows
    zhalf = slabs * rows
    zblk = 2 * zhalf
    pitch = turn.shape[0] // rows
    pairs = rows // 2
    some = pairs // 2
    s = lax.axis_index("slab")
    m = lax.axis_index("tm")

    def field_copy(xp):
        part = (slice(None), pl.ds(2 * xp, 2))
        return pltpu.make_async_copy(field_ref.at[part], fld.at[part], load_sem.at[xp])

    rest_rows = pl.ds(1, chunks - 1)
    tables = [
        pltpu.make_async_copy(a, b, table_sem.at[i])
        for i, (a, b) in enumerate(
            [
                (fwd_ref.at[0], fwd.at[0]),
                (fwd_ref.at[rest_rows], fwd.at[rest_rows]),
                (across_ref, across),
                (time_ref, wt),
                (back_ref, back),
            ]
        )
    ]
    tables[0].start()
    for xp in range(some):
        field_copy(xp).start()

    half = times // 2
    side = m // half
    cross = [(1 - side) * half + i for i in range(half)]
    near = [side * half + (m + i) % half for i in range(1, half)]
    line = cross + near
    line_home = cross[:1] + near + cross[1:]
    ring = [(s + k) % slabs for k in range(1, slabs)]

    barrier = pltpu.get_barrier_semaphore()
    for k in range(1, times):

        @pl.when(m + k < times)
        def _():
            pl.semaphore_signal(barrier, inc=1, device_id=(s, m + k), device_id_type=MESH)

    for k in range(1, slabs):

        @pl.when(s + k < slabs)
        def _():
            pl.semaphore_signal(barrier, inc=1, device_id=(s + k, m), device_id_type=MESH)

    def answer():
        @pl.when(m + s > 0)
        def _():
            pl.semaphore_wait(barrier, m + s)

        for k in range(1, times):

            @pl.when(m >= k)
            def _():
                pl.semaphore_signal(
                    line_ready.at[m], inc=1, device_id=(s, m - k), device_id_type=MESH
                )

        for k in range(1, slabs):

            @pl.when(s >= k)
            def _():
                pl.semaphore_signal(
                    ring_ready.at[s], inc=1, device_id=(s - k, m), device_id_type=MESH
                )

    def await_line(there):
        @pl.when(there > m)
        def _():
            pl.semaphore_wait(line_ready.at[there], 1)

    def await_ring(there):
        @pl.when(there > s)
        def _():
            pl.semaphore_wait(ring_ready.at[there], 1)

    def remote(src, dst, first, second, device):
        return pltpu.make_async_remote_copy(
            src_ref=src,
            dst_ref=dst,
            send_sem=first,
            recv_sem=second,
            device_id=device,
            device_id_type=MESH,
        )

    def whole(ref, first, second):
        return remote(ref, ref, first, second, (s, m))

    def out_along_t(c, first, count, peers):
        for there in peers:
            remote(
                zsend.at[c, pl.ds(there * zblk + first, count)],
                zrecv.at[c, pl.ds(m * zblk + first, count)],
                zsend_sem.at[c],
                zrecv_sem.at[c],
                (s, there),
            ).start()

    def out_across(c):
        for there in ring:
            remote(
                asend.at[c, pl.ds(there * blk, blk)],
                arecv.at[c, pl.ds(s * blk, blk)],
                asend_sem.at[c],
                arecv_sem.at[c],
                (there, m),
            ).start()

    def home_across(c):
        for there in ring:
            remote(
                bsend.at[c, pl.ds(there * blk, blk)],
                brecv.at[c, pl.ds(s * blk, blk)],
                bsend_sem.at[c],
                brecv_sem.at[c],
                (there, m),
            ).start()

    def home_along_t(c, there, first, count, arrived):
        remote(
            hsend.at[c, pl.ds(there * zblk + first, count)],
            home.at[c, pl.ds(m * zblk + first, count)],
            hsend_sem.at[c],
            arrived,
            (s, there),
        ).start()

    z_others = pl.ds(0, (times - 1) * zblk)
    z_half_others = pl.ds(0, (times - 1) * zhalf)
    a_others = pl.ds(0, (slabs - 1) * blk)

    def prepare(xp, total):
        field_copy(xp).wait()
        for q in range(2):
            value = jnp.concatenate([fld[q, 2 * xp], fld[q, 2 * xp + 1]], axis=1)
            high, low = split(value)
            fh[xp, pl.ds(q * ny, ny), :] = high
            fl[xp, pl.ds(q * ny, ny), :] = low
            total = total + jnp.sum((value * value).reshape(ny // 8, 8, 2 * cols), axis=0)
        return total

    def along_y(c, xp):
        result = left_table(fwd[c], fh[xp], fl[xp])
        turn[pl.ds(2 * xp * pitch, 2 * group), :] = result[:, :cols]
        turn[pl.ds((2 * xp + 1) * pitch, 2 * group), :] = result[:, cols:]

    def lay_out(c, h):
        for there in range(times):
            for k in range(slabs):
                for q in range(2):
                    zsend[c, pl.ds(there * zblk + h * zhalf + k * rows + q * 8, 8), :] = turn[
                        pl.ds(h * 8 * pitch + q * group + there * slabs + k, 8, stride=pitch), :
                    ]
        mine = pl.ds(m * zblk + h * zhalf, zhalf)
        zrecv[c, mine, :] = zsend[c, mine, :]

    total = jnp.zeros((8, 2 * cols), jnp.float32)
    for h in range(2):
        for xp in range(h * some, (h + 1) * some):
            total = prepare(xp, total)
            if xp < some:
                field_copy(some + xp).start()
        if h == 0:
            answer()
            tables[0].wait()
        else:
            for copy in tables[1:]:
                copy.start()
            tile = jnp.sum(total[:, :cols] + total[:, cols:], axis=0, keepdims=True)
            pw_send[0] = tile
            pw_recv[s] = tile
        for xp in range(h * some, (h + 1) * some):
            along_y(0, xp)
        lay_out(0, h)
        if h == 0:
            await_line(line[0])
            out_along_t(0, 0, zhalf, line[:1])
        else:
            for there in line[1:]:
                await_line(there)
            out_along_t(0, 0, zhalf, line[1:])
            out_along_t(0, zhalf, zhalf, line)
    for there in ring:
        await_ring(there)
        remote(pw_send.at[0], pw_recv.at[s], pw_sem.at[0], pw_sem.at[1], (there, m)).start()
    slab_tiles = pw_recv.at[pl.ds(0, slabs - 1)]
    whole(slab_tiles, pw_sem.at[0], pw_sem.at[1]).wait_recv()
    tile = jnp.sum(pw_recv[...], axis=0)
    pw_send[1] = tile
    pw_all[m] = tile
    for there in line:
        remote(pw_send.at[1], pw_all.at[m], pw_sem.at[2], pw_sem.at[3], (s, there)).start()
    tables[1].wait()

    def rest(c, carry):
        def body(xp, inner):
            along_y(c, xp)
            return inner

        lax.fori_loop(0, pairs, body, 0)
        for h in range(2):
            lay_out(c, h)
        out_along_t(c, 0, zblk, line)
        return carry

    lax.fori_loop(1, chunks, rest, 0)

    for copy in tables[2:]:
        copy.wait()
    line_tiles = pw_all.at[pl.ds(0, times - 1)]
    whole(line_tiles, pw_sem.at[2], pw_sem.at[3]).wait_recv()
    power = jnp.sum(jnp.sum(pw_all[...], axis=0), axis=(0, 1), keepdims=True)
    scale = 1.0 / jnp.sqrt(power / (nx * ny * nt) + EPSILON)
    sets = 2 * slabs
    position = lax.broadcasted_iota(jnp.int32, (sets, 8, WIDE), 0) * 8
    position = position + lax.broadcasted_iota(jnp.int32, (sets, 8, WIDE), 1)
    place_x = place(position, nx)
    square_x = place_x * place_x
    tiles = nt // WIDE
    per_tile = WIDE // cols

    def parts_of(value):
        value = value.reshape(sets, 2, 8, WIDE)
        return value[:, 0], value[:, 1]

    def along_t(n):
        lanes = pl.ds(n * WIDE, WIDE)
        products = []
        for part in range(2):
            both = dot(ysp[...], wt[part, 0, :, lanes])
            low = dot(ysp[: 2 * nx], wt[part, 1, :, lanes])
            products.append(parts_of(both[: 2 * nx] + both[2 * nx :] + low))
        (rr, ir), (ri, ii) = products
        return rr - ii, ri + ir

    def first_t(c):
        whole(zrecv.at[c, z_others], zsend_sem.at[c], zrecv_sem.at[c]).wait_recv()
        for b in range(times):
            high, low = split(zrecv[c, pl.ds(b * zblk, zblk), :])
            ysp[pl.ds(0, 2 * nx), pl.ds(b * cols, cols)] = high
            ysp[pl.ds(2 * nx, 2 * nx), pl.ds(b * cols, cols)] = low
        for n in range(tiles):
            lanes = pl.ds(n * WIDE, WIDE)
            for q, value in enumerate(along_t(n)):
                for h in range(2):
                    for k in range(slabs):
                        asend[c, pl.ds(k * blk + h * rows + q * 8, 8), lanes] = value[h * slabs + k]
        mine = pl.ds(s * blk, blk)
        arecv[c, mine, :] = asend[c, mine, :]
        out_across(c)

    def centre(c):
        whole(arecv.at[c, a_others], asend_sem.at[c], arecv_sem.at[c]).wait_recv()
        y = c * group + m * slabs + s
        place_y = (y.astype(jnp.float32) - (ny - 1) / 2.0) / (ny / 2.0)
        well_depth = WELL * (square_x + place_y * place_y)
        for n in range(tiles):
            lanes = pl.ds(n * WIDE, WIDE)
            real, imag = parts_of(left_table(across[...], *split(arecv[c, :, lanes])))
            real, imag = kick(real, imag, scale, well_depth)
            value = jnp.stack([real, imag], axis=1).reshape(2 * nx, WIDE)
            bsend[c, :, lanes] = left_table(across[...], *split(value))
        mine = pl.ds(s * blk, blk)
        brecv[c, mine, :] = bsend[c, mine, :]
        home_across(c)

    def second_t(c):
        whole(brecv.at[c, a_others], bsend_sem.at[c], brecv_sem.at[c]).wait_recv()
        high, low = split(brecv[c])
        ysp[pl.ds(0, 2 * nx), :] = high
        ysp[pl.ds(2 * nx, 2 * nx), :] = low
        for n in range(tiles):
            for q, value in enumerate(along_t(n)):
                for h in range(2):
                    for k in range(slabs):
                        for b in range(per_tile):
                            row = (n * per_tile + b) * zblk + h * zhalf + k * rows + q * 8
                            hsend[c, pl.ds(row, 8), :] = value[
                                k * 2 + h, :, b * cols : (b + 1) * cols
                            ]
        mine = pl.ds(m * zblk, zblk)
        home[c, mine, :] = hsend[c, mine, :]

        @pl.when(c < chunks - 1)
        def _():
            for there in line_home:
                home_along_t(c, there, 0, zblk, home_sem.at[c])

        @pl.when(c == chunks - 1)
        def _():
            for there in line_home:
                for h in range(2):
                    home_along_t(c, there, h * zhalf, zhalf, home_sem.at[c + h])

    def pipeline(i, carry):
        @pl.when(i < chunks)
        def _():
            first_t(i)

        @pl.when(jnp.logical_and(i >= 1, i < chunks + 1))
        def _():
            centre(i - 1)

        @pl.when(i >= 2)
        def _():
            second_t(i - 2)

        return carry

    lax.fori_loop(0, chunks + 2, pipeline, 0)

    acc[...] = jnp.zeros_like(acc)

    def add_up(c, source, h, xp, first):
        high, low = home_pair(source, h, first, slabs, times)
        value = stacked_table(back[c], high, low)
        for q in range(2):
            for i in range(2):
                part = value[q * ny : (q + 1) * ny, i * cols : (i + 1) * cols]
                acc[q, 2 * xp + i] = acc[q, 2 * xp + i] + part

    def gather(c, carry):
        source = home.at[c]
        whole(home.at[c, z_others], hsend_sem.at[c], home_sem.at[c]).wait_recv()
        for h in range(2):

            def body(k, inner):
                add_up(c, source, h, h * some + k, 2 * k)
                return inner

            lax.fori_loop(0, some, body, 0)
        return carry

    lax.fori_loop(0, chunks - 1, gather, 0)

    last = chunks - 1

    def drain(c, carry):
        whole(zsend.at[c, z_others], zsend_sem.at[c], zrecv_sem.at[c]).wait_send()
        whole(asend.at[c, a_others], asend_sem.at[c], arecv_sem.at[c]).wait_send()
        whole(bsend.at[c, a_others], bsend_sem.at[c], brecv_sem.at[c]).wait_send()
        return carry

    lax.fori_loop(0, chunks, drain, 0)
    whole(slab_tiles, pw_sem.at[0], pw_sem.at[1]).wait_send()
    whole(line_tiles, pw_sem.at[2], pw_sem.at[3]).wait_send()

    def drain_home(c, carry):
        whole(hsend.at[c, z_others], hsend_sem.at[c], home_sem.at[c]).wait_send()
        return carry

    lax.fori_loop(0, last, drain_home, 0)
    whole(home.at[last, z_half_others], hsend_sem.at[last], home_sem.at[last]).wait_recv()
    for xp in range(some):
        add_up(last, home.at[last], 0, xp, 2 * xp)
    drain_home(last, 0)
    whole(home.at[last, z_half_others], hsend_sem.at[last], home_sem.at[last + 1]).wait_recv()


def finish_kernel(dims, acc, home, back, out_ref, stage, out_sem):
    slabs, times, rows, ny, cols, chunks = dims
    pairs = rows // 2
    some = pairs // 2

    def early(xp):
        part = (slice(None), pl.ds(2 * xp, 2))
        return pltpu.make_async_copy(acc.at[part], out_ref.at[part], out_sem.at[xp])

    def late(k):
        return pltpu.make_async_copy(
            stage.at[:, pl.ds(2 * k, 2)],
            out_ref.at[:, pl.ds(rows // 2 + 2 * k, 2)],
            out_sem.at[some + k],
        )

    for xp in range(some):
        early(xp).start()
    for k in range(some):
        high, low = home_pair(home.at[chunks - 1], 1, 2 * k, slabs, times)
        value = stacked_table(back[...], high, low)
        for q in range(2):
            for i in range(2):
                part = value[q * ny : (q + 1) * ny, i * cols : (i + 1) * cols]
                stage[q, 2 * k + i] = acc[q, rows // 2 + 2 * k + i] + part
        late(k).start()
    for xp in range(some):
        early(xp).wait()
    for k in range(some):
        late(k).wait()


def in_kernels(field, slabs, times):
    _, rows, ny, cols = field.shape
    group = slabs * times
    nx, nt = rows * slabs, cols * times
    chunks = ny // group
    blk = 2 * rows
    pitch = 2 * group + 8
    uy = matrix(ny, -DIFFRACT)
    ux = matrix(nx, -DIFFRACT)
    ut = matrix(nt, DISPERSE)
    full_y = blocks(uy).reshape(2, ny, 2, ny)
    fwd, back = [], []
    for c in range(chunks):
        mine = slice(c * group, (c + 1) * group)
        fwd.append(np.concatenate(halves(full_y[:, mine].reshape(2 * group, 2 * ny))))
        high, low = halves(full_y[:, :, :, mine].reshape(2 * ny, 2 * group))
        back.append(np.concatenate([high, low, high], axis=1))
    fwd, back = np.stack(fwd), np.stack(back)
    full_x = blocks(ux).reshape(2, 2 * slabs, 8, 2, 2 * slabs, 8).transpose(1, 0, 2, 4, 3, 5)
    across = np.concatenate(halves(full_x.reshape(2 * nx, 2 * nx)))
    time = np.stack([np.stack(halves(ut.real)), np.stack(halves(ut.imag))])
    dims = (slabs, times, rows, ny, cols, chunks)
    f32, bf16 = jnp.float32, jnp.bfloat16
    hbm = pl.BlockSpec(memory_space=pltpu.HBM)
    vmem = pl.BlockSpec(memory_space=pltpu.VMEM)
    dma = pltpu.SemaphoreType.DMA
    narrow = (chunks, group * blk, cols)
    wide = (chunks, slabs * blk, nt)
    tables = [jnp.asarray(a) for a in (fwd, across, time, back)]
    acc, home = pl.pallas_call(
        functools.partial(step_kernel, dims),
        out_shape=(
            jax.ShapeDtypeStruct(field.shape, f32),
            jax.ShapeDtypeStruct(narrow, f32),
        ),
        in_specs=[hbm] * 5,
        out_specs=(vmem, vmem),
        scratch_shapes=[
            pltpu.VMEM(field.shape, f32),
            pltpu.VMEM((rows // 2, 2 * ny, 2 * cols), bf16),
            pltpu.VMEM((rows // 2, 2 * ny, 2 * cols), bf16),
            pltpu.VMEM(fwd.shape, bf16),
            pltpu.VMEM(across.shape, bf16),
            pltpu.VMEM(time.shape, bf16),
            pltpu.VMEM(back.shape, bf16),
            pltpu.VMEM((rows * pitch, cols), f32),
            pltpu.VMEM(narrow, f32),
            pltpu.VMEM(narrow, f32),
            pltpu.VMEM(wide, f32),
            pltpu.VMEM(wide, f32),
            pltpu.VMEM(wide, f32),
            pltpu.VMEM(wide, f32),
            pltpu.VMEM(narrow, f32),
            pltpu.VMEM((4 * nx, nt), bf16),
            pltpu.VMEM((2, 1, cols), f32),
            pltpu.VMEM((slabs, 1, cols), f32),
            pltpu.VMEM((times, 1, cols), f32),
            dma((rows // 2,)),
            dma((5,)),
            dma((chunks,)),
            dma((chunks,)),
            dma((chunks,)),
            dma((chunks,)),
            dma((chunks,)),
            dma((chunks,)),
            dma((chunks,)),
            dma((chunks + 1,)),
            dma((4,)),
            pltpu.SemaphoreType.REGULAR((times,)),
            pltpu.SemaphoreType.REGULAR((slabs,)),
        ],
        compiler_params=pltpu.CompilerParams(
            collective_id=0, has_side_effects=True, vmem_limit_bytes=45 * 1024 * 1024
        ),
    )(field, *[pltpu.with_memory_space_constraint(a, pltpu.HBM) for a in tables])
    return pl.pallas_call(
        functools.partial(finish_kernel, dims),
        out_shape=jax.ShapeDtypeStruct(field.shape, f32),
        in_specs=[vmem] * 3,
        out_specs=hbm,
        scratch_shapes=[
            pltpu.VMEM((2, rows // 2, ny, cols), f32),
            dma((rows // 2,)),
        ],
        compiler_params=pltpu.CompilerParams(vmem_limit_bytes=16 * 1024 * 1024),
    )(acc, home, jnp.asarray(back[-1]))


def on_device(field):
    slabs = lax.axis_size("slab")
    times = lax.axis_size("tm")
    devices = slabs * times
    _, rows, ny, cols = field.shape
    nx = rows * slabs
    nt = cols * times
    if (
        ny % devices == 0
        and ny // devices > 2
        and slabs == 8
        and rows == 16
        and cols == LANES
        and nt % WIDE == 0
        and times % 2 == 0
    ):
        return in_kernels(field, slabs, times)

    along_x = propagator(nx, -DIFFRACT)
    along_y = propagator(ny, -DIFFRACT)
    along_t = propagator(nt, DISPERSE)
    partial_power = jnp.sum(field[0] * field[0] + field[1] * field[1])
    mean_power = lax.psum(partial_power, AXES) / (nx * ny * nt)
    scale = 1.0 / jnp.sqrt(mean_power + EPSILON)
    index_x = jnp.arange(nx, dtype=jnp.int32)
    group = ny // times
    width = group * nt // slabs
    sent = apply("qzpb,pabc->qazc", along_y, field)
    timed = lax.all_to_all(sent, "tm", split_axis=2, concat_axis=3, tiled=True)
    timed = apply("rtqT,qabT->rabt", along_t, timed)
    crossed = lax.all_to_all(
        timed.reshape(2, rows, slabs, width), "slab", split_axis=2, concat_axis=1, tiled=True
    ).reshape(2, nx, width)
    crossed = apply("qxpX,pXw->qxw", along_x, crossed)
    flat = lax.axis_index("slab") * width + jnp.arange(width, dtype=jnp.int32)
    place_y = place(lax.axis_index("tm") * group + flat // nt, ny)
    well_depth = WELL * (place(index_x, nx)[:, None] ** 2 + place_y[None, :] ** 2)
    kicked = jnp.stack(kick(crossed[0], crossed[1], scale, well_depth))
    kicked = apply("qxpX,pXw->qxw", along_x, kicked)
    timed = lax.all_to_all(
        kicked.reshape(2, nx, 1, width), "slab", split_axis=1, concat_axis=2, tiled=True
    ).reshape(2, rows, group, nt)
    timed = apply("rtqT,qabT->rabt", along_t, timed)
    home = lax.all_to_all(timed, "tm", split_axis=3, concat_axis=2, tiled=True)
    return apply("qzpb,pabc->qazc", along_y, home)


def solution(mesh):
    placed = (P(None, "slab", None, "tm"),)
    return jax.shard_map(
        on_device,
        mesh=mesh,
        in_specs=placed,
        out_specs=P(None, "slab", None, "tm"),
        check_vma=False,
    )
```

```python
import functools
import math

import ml_dtypes
import numpy as np

import jax
import jax.numpy as jnp
from jax import lax
from jax.experimental import pallas as pl
from jax.experimental.pallas import tpu as pltpu
from jax.sharding import PartitionSpec as P

TWO_PI = 2.0 * math.pi
DIFFRACT = 4.0
DISPERSE = 3.0
KERR = 0.05
WELL = 1.5
EPSILON = 1e-06
AXES = ("slab", "tm")
LANES = 128
WIDE = 256
MESH = pl.DeviceIdType.MESH


def matrix(length, strength):
    steps = np.arange(length)
    signed = np.where(2 * steps < length, steps, steps - length)
    phase = np.exp(1j * strength * (TWO_PI * signed / length) ** 2)
    response = np.fft.ifft(phase)
    return response[(steps[:, None] - steps[None, :]) % length]


def propagator(length, strength):
    whole = matrix(length, strength)
    real = jnp.asarray(whole.real.astype(np.float32))
    imag = jnp.asarray(whole.imag.astype(np.float32))
    upper = jnp.stack([real, -imag], axis=1)
    lower = jnp.stack([imag, real], axis=1)
    return jnp.stack([upper, lower])


def halves(table):
    table = table.astype(np.float32)
    high = table.astype(ml_dtypes.bfloat16)
    low = (table - high.astype(np.float32)).astype(ml_dtypes.bfloat16)
    return high, low


def blocks(whole):
    return np.block([[whole.real, -whole.imag], [whole.imag, whole.real]])


def apply(form, table, value):
    return jnp.einsum(form, table, value, precision=lax.Precision.HIGH)


def place(index, length):
    return (index.astype(jnp.float32) - (length - 1) / 2.0) / (length / 2.0)


def kick(real, imag, scale, well_depth):
    real = real * scale
    imag = imag * scale
    angle = KERR * (real * real + imag * imag) - well_depth
    turn_c = jnp.cos(angle)
    turn_s = jnp.sin(angle)
    return real * turn_c - imag * turn_s, real * turn_s + imag * turn_c


def split(value):
    high = value.astype(jnp.bfloat16)
    low = (value - high.astype(jnp.float32)).astype(jnp.bfloat16)
    return high, low


def dot(left, right):
    return jnp.dot(left, right, preferred_element_type=jnp.float32)


def left_table(table, high, low):
    n = table.shape[0] // 2
    both = dot(table, high)
    return both[:n] + both[n:] + dot(table[:n], low)


def stacked_table(table, high, low):
    return dot(table, jnp.concatenate([high, high, low], axis=0))


def home_pair(home, h, first, slabs, times):
    sides = []
    for i in range(2):
        pieces = []
        for q in range(2):
            for b in range(times):
                start = ((b * 2 + h) * slabs * 2 + q) * 8 + first + i
                pieces.append(home[pl.ds(start, slabs, stride=16), :])
        sides.append(jnp.concatenate(pieces, axis=0))
    return split(jnp.concatenate(sides, axis=1))


def step_kernel(
    dims,
    field_ref,
    fwd_ref,
    across_ref,
    time_ref,
    back_ref,
    acc,
    home,
    fld,
    fh,
    fl,
    fwd,
    across,
    wt,
    back,
    turn,
    zsend,
    zrecv,
    asend,
    arecv,
    bsend,
    brecv,
    hsend,
    ysp,
    pw_send,
    pw_recv,
    pw_all,
    load_sem,
    table_sem,
    zsend_sem,
    zrecv_sem,
    asend_sem,
    arecv_sem,
    bsend_sem,
    brecv_sem,
    hsend_sem,
    home_sem,
    pw_sem,
):
    slabs, times, rows, ny, cols, chunks = dims
    group = slabs * times
    nx, nt = slabs * rows, times * cols
    blk = 2 * rows
    zhalf = slabs * rows
    zblk = 2 * zhalf
    pitch = turn.shape[0] // rows
    pairs = rows // 2
    some = pairs // 2
    s = lax.axis_index("slab")
    m = lax.axis_index("tm")

    def field_copy(xp):
        part = (slice(None), pl.ds(2 * xp, 2))
        return pltpu.make_async_copy(field_ref.at[part], fld.at[part], load_sem.at[xp])

    rest_rows = pl.ds(1, chunks - 1)
    tables = [
        pltpu.make_async_copy(a, b, table_sem.at[i])
        for i, (a, b) in enumerate(
            [
                (fwd_ref.at[0], fwd.at[0]),
                (fwd_ref.at[rest_rows], fwd.at[rest_rows]),
                (across_ref, across),
                (time_ref, wt),
                (back_ref, back),
            ]
        )
    ]
    tables[0].start()
    for xp in range(some):
        field_copy(xp).start()

    half = times // 2
    side = m // half
    cross = [(1 - side) * half + i for i in range(half)]
    near = [side * half + (m + i) % half for i in range(1, half)]
    line = cross + near
    line_home = cross[:1] + near + cross[1:]
    ring = [(s + k) % slabs for k in range(1, slabs)]

    barrier = pltpu.get_barrier_semaphore()
    for there in line:
        pl.semaphore_signal(barrier, inc=1, device_id=(s, there), device_id_type=MESH)
    for there in ring:
        pl.semaphore_signal(barrier, inc=1, device_id=(there, m), device_id_type=MESH)

    def remote(src, dst, first, second, device):
        return pltpu.make_async_remote_copy(
            src_ref=src,
            dst_ref=dst,
            send_sem=first,
            recv_sem=second,
            device_id=device,
            device_id_type=MESH,
        )

    def whole(ref, first, second):
        return remote(ref, ref, first, second, (s, m))

    def out_along_t(c, first, count, peers):
        for there in peers:
            remote(
                zsend.at[c, pl.ds(there * zblk + first, count)],
                zrecv.at[c, pl.ds(m * zblk + first, count)],
                zsend_sem.at[c],
                zrecv_sem.at[c],
                (s, there),
            ).start()

    def out_across(c):
        for there in ring:
            remote(
                asend.at[c, pl.ds(there * blk, blk)],
                arecv.at[c, pl.ds(s * blk, blk)],
                asend_sem.at[c],
                arecv_sem.at[c],
                (there, m),
            ).start()

    def home_across(c):
        for there in ring:
            remote(
                bsend.at[c, pl.ds(there * blk, blk)],
                brecv.at[c, pl.ds(s * blk, blk)],
                bsend_sem.at[c],
                brecv_sem.at[c],
                (there, m),
            ).start()

    def home_along_t(c, there, first, count, arrived):
        remote(
            hsend.at[c, pl.ds(there * zblk + first, count)],
            home.at[c, pl.ds(m * zblk + first, count)],
            hsend_sem.at[c],
            arrived,
            (s, there),
        ).start()

    z_others = pl.ds(0, (times - 1) * zblk)
    z_half_others = pl.ds(0, (times - 1) * zhalf)
    a_others = pl.ds(0, (slabs - 1) * blk)

    def prepare(xp, total):
        field_copy(xp).wait()
        for q in range(2):
            value = jnp.concatenate([fld[q, 2 * xp], fld[q, 2 * xp + 1]], axis=1)
            high, low = split(value)
            fh[xp, pl.ds(q * ny, ny), :] = high
            fl[xp, pl.ds(q * ny, ny), :] = low
            total = total + jnp.sum((value * value).reshape(ny // 8, 8, 2 * cols), axis=0)
        return total

    def along_y(c, xp):
        result = left_table(fwd[c], fh[xp], fl[xp])
        turn[pl.ds(2 * xp * pitch, 2 * group), :] = result[:, :cols]
        turn[pl.ds((2 * xp + 1) * pitch, 2 * group), :] = result[:, cols:]

    def lay_out(c, h):
        for there in range(times):
            for k in range(slabs):
                for q in range(2):
                    zsend[c, pl.ds(there * zblk + h * zhalf + k * rows + q * 8, 8), :] = turn[
                        pl.ds(h * 8 * pitch + q * group + there * slabs + k, 8, stride=pitch), :
                    ]
        mine = pl.ds(m * zblk + h * zhalf, zhalf)
        zrecv[c, mine, :] = zsend[c, mine, :]

    total = jnp.zeros((8, 2 * cols), jnp.float32)
    for h in range(2):
        for xp in range(h * some, (h + 1) * some):
            total = prepare(xp, total)
            if xp < some:
                field_copy(some + xp).start()
        if h == 0:
            tables[0].wait()
        else:
            for copy in tables[1:]:
                copy.start()
            tile = jnp.sum(total[:, :cols] + total[:, cols:], axis=0, keepdims=True)
            pw_send[0] = tile
            pw_recv[s] = tile
            for there in ring:
                remote(
                    pw_send.at[0], pw_recv.at[s], pw_sem.at[0], pw_sem.at[1], (there, m)
                ).start()
        for xp in range(h * some, (h + 1) * some):
            along_y(0, xp)
        lay_out(0, h)
        if h == 0:
            pl.semaphore_wait(barrier, times - 1 + slabs - 1)
        if h == 0:
            out_along_t(0, 0, zhalf, line[:1])

            @pl.when(s % 2 == 0)
            def _():
                out_along_t(0, 0, zhalf, line[1:])
        else:

            @pl.when(s % 2 == 1)
            def _():
                out_along_t(0, 0, zhalf, line[1:])

            out_along_t(0, zhalf, zhalf, line)
    slab_tiles = pw_recv.at[pl.ds(0, slabs - 1)]
    whole(slab_tiles, pw_sem.at[0], pw_sem.at[1]).wait_recv()
    tile = jnp.sum(pw_recv[...], axis=0)
    pw_send[1] = tile
    pw_all[m] = tile
    for there in line:
        remote(pw_send.at[1], pw_all.at[m], pw_sem.at[2], pw_sem.at[3], (s, there)).start()
    tables[1].wait()

    def rest(c, carry):
        def body(xp, inner):
            along_y(c, xp)
            return inner

        lax.fori_loop(0, pairs, body, 0)
        for h in range(2):
            lay_out(c, h)
        out_along_t(c, 0, zblk, line)
        return carry

    lax.fori_loop(1, chunks, rest, 0)

    for copy in tables[2:]:
        copy.wait()
    line_tiles = pw_all.at[pl.ds(0, times - 1)]
    whole(line_tiles, pw_sem.at[2], pw_sem.at[3]).wait_recv()
    power = jnp.sum(jnp.sum(pw_all[...], axis=0), axis=(0, 1), keepdims=True)
    scale = 1.0 / jnp.sqrt(power / (nx * ny * nt) + EPSILON)
    sets = 2 * slabs
    position = lax.broadcasted_iota(jnp.int32, (sets, 8, WIDE), 0) * 8
    position = position + lax.broadcasted_iota(jnp.int32, (sets, 8, WIDE), 1)
    place_x = place(position, nx)
    square_x = place_x * place_x
    tiles = nt // WIDE
    per_tile = WIDE // cols

    def parts_of(value):
        value = value.reshape(sets, 2, 8, WIDE)
        return value[:, 0], value[:, 1]

    def along_t(n):
        lanes = pl.ds(n * WIDE, WIDE)
        products = []
        for part in range(2):
            both = dot(ysp[...], wt[part, 0, :, lanes])
            low = dot(ysp[: 2 * nx], wt[part, 1, :, lanes])
            products.append(parts_of(both[: 2 * nx] + both[2 * nx :] + low))
        (rr, ir), (ri, ii) = products
        return rr - ii, ri + ir

    def first_t(c):
        whole(zrecv.at[c, z_others], zsend_sem.at[c], zrecv_sem.at[c]).wait_recv()
        for b in range(times):
            high, low = split(zrecv[c, pl.ds(b * zblk, zblk), :])
            ysp[pl.ds(0, 2 * nx), pl.ds(b * cols, cols)] = high
            ysp[pl.ds(2 * nx, 2 * nx), pl.ds(b * cols, cols)] = low
        for n in range(tiles):
            lanes = pl.ds(n * WIDE, WIDE)
            for q, value in enumerate(along_t(n)):
                for h in range(2):
                    for k in range(slabs):
                        asend[c, pl.ds(k * blk + h * rows + q * 8, 8), lanes] = value[h * slabs + k]
        mine = pl.ds(s * blk, blk)
        arecv[c, mine, :] = asend[c, mine, :]
        out_across(c)

    def centre(c):
        whole(arecv.at[c, a_others], asend_sem.at[c], arecv_sem.at[c]).wait_recv()
        y = c * group + m * slabs + s
        place_y = (y.astype(jnp.float32) - (ny - 1) / 2.0) / (ny / 2.0)
        well_depth = WELL * (square_x + place_y * place_y)
        for n in range(tiles):
            lanes = pl.ds(n * WIDE, WIDE)
            real, imag = parts_of(left_table(across[...], *split(arecv[c, :, lanes])))
            real, imag = kick(real, imag, scale, well_depth)
            value = jnp.stack([real, imag], axis=1).reshape(2 * nx, WIDE)
            bsend[c, :, lanes] = left_table(across[...], *split(value))
        mine = pl.ds(s * blk, blk)
        brecv[c, mine, :] = bsend[c, mine, :]
        home_across(c)

    def second_t(c):
        whole(brecv.at[c, a_others], bsend_sem.at[c], brecv_sem.at[c]).wait_recv()
        high, low = split(brecv[c])
        ysp[pl.ds(0, 2 * nx), :] = high
        ysp[pl.ds(2 * nx, 2 * nx), :] = low
        for n in range(tiles):
            for q, value in enumerate(along_t(n)):
                for h in range(2):
                    for k in range(slabs):
                        for b in range(per_tile):
                            row = (n * per_tile + b) * zblk + h * zhalf + k * rows + q * 8
                            hsend[c, pl.ds(row, 8), :] = value[
                                k * 2 + h, :, b * cols : (b + 1) * cols
                            ]
        mine = pl.ds(m * zblk, zblk)
        home[c, mine, :] = hsend[c, mine, :]

        @pl.when(c < chunks - 1)
        def _():
            for there in line_home:
                home_along_t(c, there, 0, zblk, home_sem.at[c])

        @pl.when(c == chunks - 1)
        def _():
            for there in line_home:
                for h in range(2):
                    home_along_t(c, there, h * zhalf, zhalf, home_sem.at[c + h])

    def pipeline(i, carry):
        @pl.when(i < chunks)
        def _():
            first_t(i)

        @pl.when(jnp.logical_and(i >= 1, i < chunks + 1))
        def _():
            centre(i - 1)

        @pl.when(i >= 2)
        def _():
            second_t(i - 2)

        return carry

    lax.fori_loop(0, chunks + 2, pipeline, 0)

    acc[...] = jnp.zeros_like(acc)

    def add_up(c, source, h, xp, first):
        high, low = home_pair(source, h, first, slabs, times)
        value = stacked_table(back[c], high, low)
        for q in range(2):
            for i in range(2):
                part = value[q * ny : (q + 1) * ny, i * cols : (i + 1) * cols]
                acc[q, 2 * xp + i] = acc[q, 2 * xp + i] + part

    def gather(c, carry):
        source = home.at[c]
        whole(home.at[c, z_others], hsend_sem.at[c], home_sem.at[c]).wait_recv()
        for h in range(2):

            def body(k, inner):
                add_up(c, source, h, h * some + k, 2 * k)
                return inner

            lax.fori_loop(0, some, body, 0)
        return carry

    lax.fori_loop(0, chunks - 1, gather, 0)

    last = chunks - 1

    def drain(c, carry):
        whole(zsend.at[c, z_others], zsend_sem.at[c], zrecv_sem.at[c]).wait_send()
        whole(asend.at[c, a_others], asend_sem.at[c], arecv_sem.at[c]).wait_send()
        whole(bsend.at[c, a_others], bsend_sem.at[c], brecv_sem.at[c]).wait_send()
        return carry

    lax.fori_loop(0, chunks, drain, 0)
    whole(slab_tiles, pw_sem.at[0], pw_sem.at[1]).wait_send()
    whole(line_tiles, pw_sem.at[2], pw_sem.at[3]).wait_send()

    def drain_home(c, carry):
        whole(hsend.at[c, z_others], hsend_sem.at[c], home_sem.at[c]).wait_send()
        return carry

    lax.fori_loop(0, last, drain_home, 0)
    whole(home.at[last, z_half_others], hsend_sem.at[last], home_sem.at[last]).wait_recv()
    for xp in range(some):
        add_up(last, home.at[last], 0, xp, 2 * xp)
    drain_home(last, 0)
    whole(home.at[last, z_half_others], hsend_sem.at[last], home_sem.at[last + 1]).wait_recv()


def finish_kernel(dims, acc, home, back, out_ref, stage, out_sem):
    slabs, times, rows, ny, cols, chunks = dims
    pairs = rows // 2
    some = pairs // 2

    def early(xp):
        part = (slice(None), pl.ds(2 * xp, 2))
        return pltpu.make_async_copy(acc.at[part], out_ref.at[part], out_sem.at[xp])

    def late(k):
        return pltpu.make_async_copy(
            stage.at[:, pl.ds(2 * k, 2)],
            out_ref.at[:, pl.ds(rows // 2 + 2 * k, 2)],
            out_sem.at[some + k],
        )

    for xp in range(some):
        early(xp).start()
    for k in range(some):
        high, low = home_pair(home.at[chunks - 1], 1, 2 * k, slabs, times)
        value = stacked_table(back[...], high, low)
        for q in range(2):
            for i in range(2):
                part = value[q * ny : (q + 1) * ny, i * cols : (i + 1) * cols]
                stage[q, 2 * k + i] = acc[q, rows // 2 + 2 * k + i] + part
        late(k).start()
    for xp in range(some):
        early(xp).wait()
    for k in range(some):
        late(k).wait()


def in_kernels(field, slabs, times):
    _, rows, ny, cols = field.shape
    group = slabs * times
    nx, nt = rows * slabs, cols * times
    chunks = ny // group
    blk = 2 * rows
    pitch = 2 * group + 8
    uy = matrix(ny, -DIFFRACT)
    ux = matrix(nx, -DIFFRACT)
    ut = matrix(nt, DISPERSE)
    full_y = blocks(uy).reshape(2, ny, 2, ny)
    fwd, back = [], []
    for c in range(chunks):
        mine = slice(c * group, (c + 1) * group)
        fwd.append(np.concatenate(halves(full_y[:, mine].reshape(2 * group, 2 * ny))))
        high, low = halves(full_y[:, :, :, mine].reshape(2 * ny, 2 * group))
        back.append(np.concatenate([high, low, high], axis=1))
    fwd, back = np.stack(fwd), np.stack(back)
    full_x = blocks(ux).reshape(2, 2 * slabs, 8, 2, 2 * slabs, 8).transpose(1, 0, 2, 4, 3, 5)
    across = np.concatenate(halves(full_x.reshape(2 * nx, 2 * nx)))
    time = np.stack([np.stack(halves(ut.real)), np.stack(halves(ut.imag))])
    dims = (slabs, times, rows, ny, cols, chunks)
    f32, bf16 = jnp.float32, jnp.bfloat16
    hbm = pl.BlockSpec(memory_space=pltpu.HBM)
    vmem = pl.BlockSpec(memory_space=pltpu.VMEM)
    dma = pltpu.SemaphoreType.DMA
    narrow = (chunks, group * blk, cols)
    wide = (chunks, slabs * blk, nt)
    tables = [jnp.asarray(a) for a in (fwd, across, time, back)]
    acc, home = pl.pallas_call(
        functools.partial(step_kernel, dims),
        out_shape=(
            jax.ShapeDtypeStruct(field.shape, f32),
            jax.ShapeDtypeStruct(narrow, f32),
        ),
        in_specs=[hbm] * 5,
        out_specs=(vmem, vmem),
        scratch_shapes=[
            pltpu.VMEM(field.shape, f32),
            pltpu.VMEM((rows // 2, 2 * ny, 2 * cols), bf16),
            pltpu.VMEM((rows // 2, 2 * ny, 2 * cols), bf16),
            pltpu.VMEM(fwd.shape, bf16),
            pltpu.VMEM(across.shape, bf16),
            pltpu.VMEM(time.shape, bf16),
            pltpu.VMEM(back.shape, bf16),
            pltpu.VMEM((rows * pitch, cols), f32),
            pltpu.VMEM(narrow, f32),
            pltpu.VMEM(narrow, f32),
            pltpu.VMEM(wide, f32),
            pltpu.VMEM(wide, f32),
            pltpu.VMEM(wide, f32),
            pltpu.VMEM(wide, f32),
            pltpu.VMEM(narrow, f32),
            pltpu.VMEM((4 * nx, nt), bf16),
            pltpu.VMEM((2, 1, cols), f32),
            pltpu.VMEM((slabs, 1, cols), f32),
            pltpu.VMEM((times, 1, cols), f32),
            dma((rows // 2,)),
            dma((5,)),
            dma((chunks,)),
            dma((chunks,)),
            dma((chunks,)),
            dma((chunks,)),
            dma((chunks,)),
            dma((chunks,)),
            dma((chunks,)),
            dma((chunks + 1,)),
            dma((4,)),
        ],
        compiler_params=pltpu.CompilerParams(
            collective_id=0, has_side_effects=True, vmem_limit_bytes=45 * 1024 * 1024
        ),
    )(field, *[pltpu.with_memory_space_constraint(a, pltpu.HBM) for a in tables])
    return pl.pallas_call(
        functools.partial(finish_kernel, dims),
        out_shape=jax.ShapeDtypeStruct(field.shape, f32),
        in_specs=[vmem] * 3,
        out_specs=hbm,
        scratch_shapes=[
            pltpu.VMEM((2, rows // 2, ny, cols), f32),
            dma((rows // 2,)),
        ],
        compiler_params=pltpu.CompilerParams(vmem_limit_bytes=16 * 1024 * 1024),
    )(acc, home, jnp.asarray(back[-1]))


def on_device(field):
    slabs = lax.axis_size("slab")
    times = lax.axis_size("tm")
    devices = slabs * times
    _, rows, ny, cols = field.shape
    nx = rows * slabs
    nt = cols * times
    if (
        ny % devices == 0
        and ny // devices > 2
        and slabs == 8
        and rows == 16
        and cols == LANES
        and nt % WIDE == 0
        and times % 2 == 0
    ):
        return in_kernels(field, slabs, times)

    along_x = propagator(nx, -DIFFRACT)
    along_y = propagator(ny, -DIFFRACT)
    along_t = propagator(nt, DISPERSE)
    partial_power = jnp.sum(field[0] * field[0] + field[1] * field[1])
    mean_power = lax.psum(partial_power, AXES) / (nx * ny * nt)
    scale = 1.0 / jnp.sqrt(mean_power + EPSILON)
    index_x = jnp.arange(nx, dtype=jnp.int32)
    group = ny // times
    width = group * nt // slabs
    sent = apply("qzpb,pabc->qazc", along_y, field)
    timed = lax.all_to_all(sent, "tm", split_axis=2, concat_axis=3, tiled=True)
    timed = apply("rtqT,qabT->rabt", along_t, timed)
    crossed = lax.all_to_all(
        timed.reshape(2, rows, slabs, width), "slab", split_axis=2, concat_axis=1, tiled=True
    ).reshape(2, nx, width)
    crossed = apply("qxpX,pXw->qxw", along_x, crossed)
    flat = lax.axis_index("slab") * width + jnp.arange(width, dtype=jnp.int32)
    place_y = place(lax.axis_index("tm") * group + flat // nt, ny)
    well_depth = WELL * (place(index_x, nx)[:, None] ** 2 + place_y[None, :] ** 2)
    kicked = jnp.stack(kick(crossed[0], crossed[1], scale, well_depth))
    kicked = apply("qxpX,pXw->qxw", along_x, kicked)
    timed = lax.all_to_all(
        kicked.reshape(2, nx, 1, width), "slab", split_axis=1, concat_axis=2, tiled=True
    ).reshape(2, rows, group, nt)
    timed = apply("rtqT,qabT->rabt", along_t, timed)
    home = lax.all_to_all(timed, "tm", split_axis=3, concat_axis=2, tiled=True)
    return apply("qzpb,pabc->qazc", along_y, home)


def solution(mesh):
    placed = (P(None, "slab", None, "tm"),)
    return jax.shard_map(
        on_device,
        mesh=mesh,
        in_specs=placed,
        out_specs=P(None, "slab", None, "tm"),
        check_vma=False,
    )
```
